128 devices in a mesh: lat: 8 (over z, core), lon: 16 (over x, y).
Axes of the slice: x: 4, y: 4, z: 4, core: 2. Of those that a mesh axis runs over, the one named last changes fastest.
Arguments:
- grid_nodes: bfloat16 [131072, 512], P(('lat', 'lon')), may hold values from -6 to 6
- grid_edges: bfloat16 [36864, 512], P(('lat', 'lon')), may hold values from -6 to 6
- grid_sender: int32 [36864], P(('lat', 'lon')), may hold values from 0 to 1023, as said below
- owner_index: int32 [36864], P(('lat', 'lon')), may hold values from -1 to 255, as said below
- mesh_nodes: bfloat16 [32768, 512], P(('lat', 'lon')), may hold values from -6 to 6
- mesh_edges: bfloat16 [65536, 512], P(('lat', 'lon')), may hold values from -6 to 6
- mesh_sender: int32 [65536], P(('lat', 'lon')), may hold values from 0 to 1023, as said below
- mesh_receiver: int32 [65536], P(('lat', 'lon')), may hold values from 0 to 255
- w_first: bfloat16 [3, 1536, 512], replicated, may hold values from -0.15625 to 0.15625
- first_bias: float32 [3, 512], replicated, may hold values from -3 to 3
- w_second: bfloat16 [3, 512, 512], replicated, may hold values from -0.25 to 0.25
- norm_gain: float32 [3, 512], replicated, may hold values from 0.25 to 1.75
- mesh_cotangent: bfloat16 [32768, 512], P(('lat', 'lon')), may hold values from -0.01953125 to 0.01953125
- edge_cotangent: bfloat16 [65536, 512], P(('lat', 'lon')), may hold values from -0.01953125 to 0.01953125
Outputs:
- updated_mesh: bfloat16 [32768, 512], P(('lat', 'lon'))
- updated_edges: bfloat16 [65536, 512], P(('lat', 'lon'))
- grad_first: float32 [3, 1536, 512], P(None, 'lat', 'lon')
- grad_second: float32 [3, 512, 512], P(None, 'lat', 'lon')
The draws below stay inside these ranges and needn't reach their ends.
Inputs may be any that keep to these rules, and one draw needn't show every extreme that they name: `grid_sender`: rows of device p, in 9 blocks of 32 by destination offset as in the reference program: the sending grid point (local index) of each slot; entries of unused slots are arbitrary. `owner_index`: rows of device q, in 9 blocks of 32 by source offset as in the reference program, matching the sender's slots: the receiving local mesh node, -1 for an unused slot. The used slots of a block come first. Blocks from beyond the first or last latitude band are unused. Some device receives 32 used slots from every device that sends to it. `mesh_sender`: row of the sender table described in the reference program; no edge refers to a lat neighbour that does not exist.
All inputs are finite; a program needn't handle non-finite values.
Results may differ from the reference program's by a relative error of at most 0.02.
Values may be sent and summed in bfloat16 or wider, within the bound.
No kernel may reach another device: no remote copies, remote signals or barrier semaphores. Data moves between devices by JAX's collectives and lax.ppermute only.
A program may use at most 128 MiB of HBM per device.

```python
import jax
import jax.numpy as jnp
from jax import lax

D = 512
FIN = 1536
G_DEV = 1024
M_DEV = 256
CAP = 32
E_M = 512
BORDER = 64
K_COARSE = 4
SLOTS_DEV = 288
GRID = 131072
MESH = 32768
SLOTS = 36864
EDGES = 65536
COARSE = 512
N_LAT = 8
N_LON = 16
DEVICES = 128


def slot_table(key):
    folded = jax.random.fold_in(key, 7101)
    keys = jax.random.split(folded, 5)
    device = jnp.arange(DEVICES, dtype=jnp.int32)
    band_index = device // N_LON
    cycle_index = device % N_LON
    offset = jnp.arange(9, dtype=jnp.int32)
    band_step = offset // 3 - 1
    cycle_step = offset % 3 - 1
    target_band = band_index[:, None] + band_step[None, :]
    exists = (target_band >= 0) & (target_band < N_LAT)
    destination = (target_band + N_LAT) % N_LAT * N_LON + (cycle_index[:, None] + cycle_step[None, :] + N_LON) % N_LON
    pair_counts = jax.random.randint(keys[0], (DEVICES, 9), 0, CAP + 1)
    owner_limit = jax.random.randint(keys[1], (DEVICES,), CAP // 2, CAP + 1)
    pair_counts = jnp.minimum(pair_counts, jnp.take(owner_limit, destination))
    full_owner = jax.random.randint(keys[2], (), 0, DEVICES)
    pair_counts = jnp.where(destination == full_owner, CAP, pair_counts)
    pair_counts = jnp.where(exists, pair_counts, 0)
    is_live = jnp.arange(CAP, dtype=jnp.int32)[None, None, :] < pair_counts[:, :, None]
    sender = jax.random.randint(keys[3], (DEVICES, 9, CAP), 0, G_DEV)
    target = jax.random.randint(keys[4], (DEVICES, 9, CAP), 0, M_DEV)
    return (is_live, sender, target)


def draw_grid_sender(key, part):
    is_live, sender, target = slot_table(key)
    return sender.reshape(-1).astype(jnp.int32)


def draw_owner_index(key, part):
    is_live, sender, target = slot_table(key)
    marked = jnp.where(is_live, target, -1)
    device = jnp.arange(DEVICES, dtype=jnp.int32)
    band_index = device // N_LON
    cycle_index = device % N_LON
    offset = jnp.arange(9, dtype=jnp.int32)
    band_step = offset // 3 - 1
    cycle_step = offset % 3 - 1
    source = (band_index[:, None] + band_step[None, :] + N_LAT) % N_LAT * N_LON + (cycle_index[:, None] + cycle_step[None, :] + N_LON) % N_LON
    flat_index = source * 9 + (8 - offset)[None, :]
    picked = jnp.take(marked.reshape(DEVICES * 9, CAP), flat_index.reshape(-1), axis=0)
    return picked.reshape(-1).astype(jnp.int32)


def draw_mesh_sender(key, part):
    folded = jax.random.fold_in(key, 7202)
    keys = jax.random.split(folded, 6)
    row_count = DEVICES * E_M
    device = jnp.arange(row_count, dtype=jnp.int32) // E_M
    band_index = device // N_LON
    choose_kind = jax.random.randint(keys[0], (row_count,), 0, 100)
    own_pick = jax.random.randint(keys[1], (row_count,), 0, M_DEV)
    border_pick = jax.random.randint(keys[2], (row_count,), 0, BORDER)
    band_side = jax.random.randint(keys[3], (row_count,), 0, 2)
    cycle_side = jax.random.randint(keys[4], (row_count,), 0, 2)
    coarse_pick = jax.random.randint(keys[5], (row_count,), 0, COARSE)
    band_exists = jnp.where(band_side == 0, band_index > 0, band_index < N_LAT - 1)
    band_row = M_DEV + band_side * BORDER + border_pick
    cycle_row = M_DEV + 2 * BORDER + cycle_side * BORDER + border_pick
    coarse_row = M_DEV + 4 * BORDER + coarse_pick
    picked = jnp.where(choose_kind < 55, own_pick, jnp.where(choose_kind < 70, jnp.where(band_exists, band_row, own_pick), jnp.where(choose_kind < 85, cycle_row, coarse_row)))
    return picked.astype(jnp.int32)


def set_ends(result, rng, least, largest):
    shape = result.shape
    spot = [jax.random.randint(jax.random.fold_in(rng, axis), (), 0, shape[axis]) for axis in range(len(shape))]
    result = result.at[tuple(spot)].set(least)
    longest = shape.index(max(shape))
    spot[longest] = (spot[longest] + 1) % shape[longest]
    return result.at[tuple(spot)].set(largest)


def levels(stream_key, dims, shards, least, largest):
    gain, own = 1.0, jax.random.fold_in(stream_key, 6)
    for axis_at, shards_of in shards:
        heights = jnp.exp(jax.random.uniform(jax.random.fold_in(own, axis_at), (shards_of,), jnp.float32, least / len(shards), largest / len(shards)))
        gain = gain * jnp.repeat(heights, dims[axis_at] // shards_of).reshape([-1 if axis == axis_at else 1 for axis in range(len(dims))])
    return gain


def scatter_about(stream_key, dims, scale, limit, pieces=(), kind=jnp.bfloat16):
    entries = scale * jax.random.normal(stream_key, dims, jnp.float32)
    if pieces:
        entries = entries * levels(stream_key, dims, pieces, -0.22, 0.18)
    return jnp.clip(entries, -limit, limit).astype(kind)


def setup_inputs(seed: int = 0) -> dict:
    arg_keys = jax.random.split(jax.random.key(seed), 15)
    return {
        "grid_nodes": scatter_about(arg_keys[0], (GRID, D), 1.0, 6.0, ((0, 128),)),
        "grid_edges": scatter_about(arg_keys[1], (SLOTS, D), 1.0, 6.0, ((0, 128),)),
        "grid_sender": draw_grid_sender(jax.random.fold_in(arg_keys[14], 71), 0),
        "owner_index": draw_owner_index(jax.random.fold_in(arg_keys[14], 71), 0),
        "mesh_nodes": scatter_about(arg_keys[4], (MESH, D), 1.0, 6.0, ((0, 128),)),
        "mesh_edges": scatter_about(arg_keys[5], (EDGES, D), 1.0, 6.0, ((0, 128),)),
        "mesh_sender": draw_mesh_sender(jax.random.fold_in(arg_keys[14], 71), 0),
        "mesh_receiver": set_ends(jax.random.randint(arg_keys[7], (EDGES,), 0, M_DEV), jax.random.fold_in(arg_keys[7], 1), 0, M_DEV - 1).astype(jnp.int32),
        "w_first": scatter_about(arg_keys[8], (3, FIN, D), FIN ** -0.5, 0.15625),
        "first_bias": scatter_about(arg_keys[9], (3, D), 0.5, 3.0, (), jnp.float32),
        "w_second": scatter_about(arg_keys[10], (3, D, D), D ** -0.5, 0.25),
        "norm_gain": jnp.clip(1.0 + 0.15 * jax.random.normal(arg_keys[11], (3, D), jnp.float32), 0.25, 1.75),
        "mesh_cotangent": scatter_about(arg_keys[12], (MESH, D), ((M_DEV + E_M) * DEVICES) ** -0.5, 0.01953125, ((0, 128),)),
        "edge_cotangent": scatter_about(arg_keys[13], (EDGES, D), ((M_DEV + E_M) * DEVICES) ** -0.5, 0.01953125, ((0, 128),)),
    }


EPSILON = 1e-05

def perceptron(inputs, weights, member, pre_shift, out_shift):
    w_first, first_bias, w_second, norm_gain = weights
    preact = jnp.dot(inputs, w_first[member], preferred_element_type=jnp.float32) + first_bias[member] + pre_shift
    hidden = jax.nn.silu(preact).astype(jnp.bfloat16)
    output = jnp.dot(hidden, w_second[member], preferred_element_type=jnp.float32) + out_shift
    centre = lax.optimization_barrier(jnp.mean(output, axis=-1, keepdims=True))
    spread = lax.optimization_barrier(jnp.mean(jnp.square(output - centre), axis=-1, keepdims=True))
    return ((output - centre) * lax.rsqrt(spread + EPSILON) * norm_gain[member], hidden)

def node_sums(receivers, messages, node_count):
    onehot = (receivers[:, None] == jnp.arange(node_count, dtype=jnp.int32)[None, :]).astype(jnp.bfloat16)
    summed = lax.dot_general(onehot, messages, (((0,), (0,)), ((), ())), preferred_element_type=jnp.float32)
    return summed.astype(jnp.bfloat16)

def layer_pass(sender_grid, grid_edge_rows, owner_rows, own_nodes, sender_table, edge_rows, edge_senders, edge_receivers, weights, shifts):
    node_count = own_nodes.shape[0]
    clipped = jnp.maximum(owner_rows, 0)
    grid_input = jnp.concatenate([grid_edge_rows, sender_grid, jnp.take(own_nodes, clipped, axis=0)], axis=1)
    grid_message, grid_hidden = perceptron(grid_input, weights, 0, shifts[0], shifts[1])
    grid_sum = node_sums(owner_rows, grid_message.astype(jnp.bfloat16), node_count)
    edge_input = jnp.concatenate([edge_rows, jnp.take(sender_table, edge_senders, axis=0), jnp.take(own_nodes, edge_receivers, axis=0)], axis=1)
    edge_message, edge_hidden = perceptron(edge_input, weights, 1, shifts[2], shifts[3])
    updated_edges = (edge_rows.astype(jnp.float32) + edge_message).astype(jnp.bfloat16)
    edge_sum = node_sums(edge_receivers, edge_message.astype(jnp.bfloat16), node_count)
    node_input = jnp.concatenate([own_nodes, grid_sum, edge_sum], axis=1)
    node_output, node_hidden = perceptron(node_input, weights, 2, shifts[4], shifts[5])
    updated_mesh = (own_nodes.astype(jnp.float32) + node_output).astype(jnp.bfloat16)
    stored = ((grid_input, grid_hidden), (edge_input, edge_hidden), (node_input, node_hidden))
    return ((updated_mesh, updated_edges), stored)

def forward_backward(sender_grid, grid_edge_rows, owner_rows, own_nodes, sender_table, edge_rows, edge_senders, edge_receivers, weights, mesh_cot, edge_cot):
    feature_width = own_nodes.shape[1]
    row_counts = (owner_rows.shape[0], owner_rows.shape[0], edge_senders.shape[0], edge_senders.shape[0], own_nodes.shape[0], own_nodes.shape[0])
    shifts = tuple((jnp.zeros((row_count, feature_width), jnp.float32) for row_count in row_counts))

    def run_layer(shift_list):
        return layer_pass(sender_grid, grid_edge_rows, owner_rows, own_nodes, sender_table, edge_rows, edge_senders, edge_receivers, weights, shift_list)
    outputs, pullback, stored = jax.vjp(run_layer, shifts, has_aux=True)
    shift_grads = pullback((mesh_cot, edge_cot))[0]
    firsts = []
    seconds = []
    for member in range(3):
        inputs, hidden = stored[member]
        pre_grad = shift_grads[2 * member].astype(jnp.bfloat16)
        out_grad = shift_grads[2 * member + 1].astype(jnp.bfloat16)
        firsts.append(lax.dot_general(inputs, pre_grad, (((0,), (0,)), ((), ())), preferred_element_type=jnp.float32))
        seconds.append(lax.dot_general(hidden, out_grad, (((0,), (0,)), ((), ())), preferred_element_type=jnp.float32))
    return (outputs[0], outputs[1], jnp.stack(firsts), jnp.stack(seconds))

def reference(grid_nodes, grid_edges, grid_sender, owner_index, mesh_nodes, mesh_edges, mesh_sender, mesh_receiver, w_first, first_bias, w_second, norm_gain, mesh_cotangent, edge_cotangent):
    weights = (w_first, first_bias, w_second, norm_gain)
    grid_blocks = grid_nodes.reshape(DEVICES, G_DEV, D)
    edge_blocks = grid_edges.reshape(DEVICES, 9, CAP, D)
    sender_blocks = grid_sender.reshape(DEVICES, 9, CAP)
    owner_blocks = owner_index.reshape(DEVICES, SLOTS_DEV)
    node_blocks = mesh_nodes.reshape(DEVICES, M_DEV, D)
    coarse_rows = node_blocks[:, M_DEV - K_COARSE:].reshape(COARSE, D)
    mesh_edge_blocks = mesh_edges.reshape(DEVICES, E_M, D)
    mesh_sender_blocks = mesh_sender.reshape(DEVICES, E_M)
    mesh_receiver_blocks = mesh_receiver.reshape(DEVICES, E_M)
    mesh_cot_blocks = mesh_cotangent.reshape(DEVICES, M_DEV, D)
    edge_cot_blocks = edge_cotangent.reshape(DEVICES, E_M, D)

    def border_of(device):
        return lax.dynamic_index_in_dim(node_blocks, device, 0, False)[:BORDER]

    def per_device(totals, device):
        band_index = device // N_LON
        cycle_index = device % N_LON
        edge_parts = []
        grid_parts = []
        for offset in range(9):
            band_step = offset // 3 - 1
            cycle_step = offset % 3 - 1
            source = (band_index + band_step + N_LAT) % N_LAT * N_LON + (cycle_index + cycle_step + N_LON) % N_LON
            source_edges = lax.dynamic_index_in_dim(edge_blocks, source, 0, False)[8 - offset]
            source_senders = lax.dynamic_index_in_dim(sender_blocks, source, 0, False)[8 - offset]
            source_grid = lax.dynamic_index_in_dim(grid_blocks, source, 0, False)
            edge_parts.append(source_edges)
            grid_parts.append(jnp.take(source_grid, source_senders, axis=0))
        grid_edge_rows = jnp.concatenate(edge_parts, axis=0)
        sender_grid = jnp.concatenate(grid_parts, axis=0)
        owner_rows = lax.dynamic_index_in_dim(owner_blocks, device, 0, False)
        own_nodes = lax.dynamic_index_in_dim(node_blocks, device, 0, False)
        lower = border_of(jnp.maximum(device - N_LON, 0))
        lower = jnp.where(band_index > 0, lower, jnp.zeros_like(lower))
        upper = border_of(jnp.minimum(device + N_LON, DEVICES - 1))
        upper = jnp.where(band_index < N_LAT - 1, upper, jnp.zeros_like(upper))
        western = border_of(band_index * N_LON + (cycle_index + N_LON - 1) % N_LON)
        eastern = border_of(band_index * N_LON + (cycle_index + 1) % N_LON)
        sender_table = jnp.concatenate([own_nodes, lower, upper, western, eastern, coarse_rows], axis=0)
        updated_mesh, updated_edges, first_term, second_term = forward_backward(sender_grid, grid_edge_rows, owner_rows, own_nodes, sender_table, lax.dynamic_index_in_dim(mesh_edge_blocks, device, 0, False), lax.dynamic_index_in_dim(mesh_sender_blocks, device, 0, False), lax.dynamic_index_in_dim(mesh_receiver_blocks, device, 0, False), weights, lax.dynamic_index_in_dim(mesh_cot_blocks, device, 0, False), lax.dynamic_index_in_dim(edge_cot_blocks, device, 0, False))
        return ((totals[0] + first_term, totals[1] + second_term), (updated_mesh, updated_edges))
    devices = jnp.arange(DEVICES, dtype=jnp.int32)
    initial = (jnp.zeros((3, FIN, D), jnp.float32), jnp.zeros((3, D, D), jnp.float32))
    totals, (mesh_rows, edge_rows) = lax.scan(per_device, initial, devices)
    return (mesh_rows.reshape(MESH, D), edge_rows.reshape(EDGES, D), totals[0], totals[1])
```

```python
import jax
import jax.numpy as jnp
from jax import lax
from jax.experimental import pallas as pl
from jax.experimental.pallas import tpu as pltpu
from jax.sharding import Mesh
from jax.sharding import PartitionSpec as P

D = 512
CAP = 32
BORDER = 64
K_COARSE = 4
EPSILON = 1e-05
ALL = ("z", "c", "x", "y")
LAT = ("z", "c")
LON = ("x", "y")
F32 = jnp.float32
BF16 = jnp.bfloat16


OFFSETS = [(a, b) for a in (-1, 0, 1) for b in (-1, 0, 1)]
MOVED = [o for o in OFFSETS if o != (0, 0)]


def number(offset):
    return 3 * (offset[0] + 1) + offset[1] + 1


def has_border(offset):
    return abs(offset[0]) + abs(offset[1]) == 1


def neighbour_pairs(offset, lats, lons):
    pairs = []
    for lat in range(lats):
        for lon in range(lons):
            to = lat + offset[0]
            if 0 <= to < lats:
                pairs.append((lat * lons + lon, to * lons + (lon + offset[1]) % lons))
    return pairs


def dot(a, b):
    return jnp.dot(a, b, preferred_element_type=F32)


def dot_nt(a, b):
    return lax.dot_general(a, b, (((1,), (1,)), ((), ())), preferred_element_type=F32)


def dot_tn(a, b):
    return lax.dot_general(a, b, (((0,), (0,)), ((), ())), preferred_element_type=F32)


def down_onehot(index, count):
    lines = lax.broadcasted_iota(jnp.int32, (count, index.shape[1]), 0)
    return jnp.where(lines == index, 1.0, 0.0).astype(BF16)


def table_row(place, row):
    first = 512
    at = row - first
    device = at >> 2
    y = (place[3] - device) & 3
    x = (place[2] - (device >> 2)) & 3
    c = (place[0] - (device >> 4)) & 1
    z = (place[1] - (device >> 5)) & 3
    moved = (((c * 4 + z) * 4 + x) * 4 + y) * 4 + (at & 3)
    return jnp.where(row < first, row, first + moved)


def pack_kernel(points, slot_edges, senders, nodes, *out):
    picked = dot_tn(down_onehot(senders[...], points.shape[0]), points[...]).astype(BF16)
    at = 0
    for offset in OFFSETS:
        o = number(offset)
        out[o][0:CAP, :] = slot_edges[o * CAP : (o + 1) * CAP, :]
        out[o][CAP : 2 * CAP, :] = picked[o * CAP : (o + 1) * CAP, :]
        if has_border(offset):
            out[o][2 * CAP : 2 * CAP + BORDER, :] = nodes[0:BORDER, :]


def packets(points, slot_edges, senders, nodes):
    shapes = [
        jax.ShapeDtypeStruct((2 * CAP + (BORDER if has_border(o) else 0), D), BF16)
        for o in OFFSETS
    ]
    return pl.pallas_call(
        pack_kernel,
        out_shape=shapes,
        name="pack",
        cost_estimate=pl.CostEstimate(
            flops=2 * 288 * 1024 * 512, bytes_accessed=2 << 20, transcendentals=0
        ),
    )(points, slot_edges, senders, nodes)


def layer_kernel(
    core,
    slots_in,
    coarse,
    owner,
    edge_sender,
    edge_receiver,
    nodes,
    edges,
    w_first,
    first_bias,
    w_second,
    norm_gain,
    mesh_cot,
    edge_cot,
    updated_mesh,
    updated_edges,
    keep,
    send,
    table,
    x_grid,
    x_edge,
    x_node,
    slope_grid,
    slope_edge,
    slope_node,
    hid_grid,
    hid_edge,
    hid_node,
    norm_grid,
    norm_edge,
    norm_node,
):
    n_nodes = nodes.shape[0]

    def forward(k, x, slope, hid, norm):
        pre = dot(x[...], w_first[k]) + first_bias[k : k + 1, :]
        sig = 0.5 + 0.5 * jnp.tanh(0.5 * pre)
        act = pre * sig
        hid[...] = act.astype(BF16)
        slope[...] = sig + act * (1.0 - sig)
        out = dot(hid[...], w_second[k])
        out = out - jnp.mean(out, axis=1, keepdims=True)
        scale = lax.rsqrt(jnp.mean(out * out, axis=1, keepdims=True) + EPSILON)
        unit = out * scale
        norm[...] = unit
        return unit * norm_gain[k : k + 1, :], scale

    def backward(k, dy, scale, slope, norm):
        unit = norm[...]
        dn = dy * norm_gain[k : k + 1, :]
        mid = jnp.mean(dn, axis=1, keepdims=True)
        along = jnp.mean(dn * unit, axis=1, keepdims=True)
        d_out = (scale * (dn - mid - unit * along)).astype(BF16)
        d_hid = dot_nt(d_out, w_second[k]).astype(BF16)
        d_pre = (d_hid.astype(F32) * slope[...]).astype(BF16)
        return d_pre, d_out

    odd = core[0] == 1
    low = lax.broadcasted_iota(jnp.int32, (D, 128), 1) < 64

    def weight_grads(k, x, hid, d_pre, d_out):
        second = dot_tn(d_out, hid[...])
        for z in range(4):
            first = dot_tn(d_pre, x[:, 384 * z : 384 * (z + 1)])
            turned = pltpu.roll(second[:, 128 * z : 128 * (z + 1)], 64, 1)
            middle = first[:, 128:256]
            even_a, odd_a = first[:, 0:128], first[:, 256:384]
            even_b = jnp.where(low, middle, turned)
            odd_b = jnp.where(low, turned, middle)
            for ref, a, b in (
                (keep, jnp.where(odd, odd_a, even_a), jnp.where(odd, odd_b, even_b)),
                (send, jnp.where(odd, even_a, odd_a), jnp.where(odd, even_b, odd_b)),
            ):
                ref[16 * z : 16 * (z + 1), k, :, 0:128] = a.astype(BF16).reshape(16, 32, 128)
                ref[16 * z : 16 * (z + 1), k, :, 128:256] = b.astype(BF16).reshape(16, 32, 128)

    for block in range(9):
        rows = slice(block * CAP, (block + 1) * CAP)
        x_grid[rows, 0:D] = slots_in[block][0:CAP, :]
        x_grid[rows, D : 2 * D] = slots_in[block][CAP : 2 * CAP, :]
    owner_hot = down_onehot(owner[...], n_nodes)
    receiver_hot = down_onehot(edge_receiver[...], n_nodes)
    x_grid[:, 2 * D :] = dot_tn(owner_hot, nodes[...]).astype(BF16)
    y_grid, scale_grid = forward(0, x_grid, slope_grid, hid_grid, norm_grid)
    x_node[:, 0:D] = nodes[...]
    x_node[:, D : 2 * D] = dot(owner_hot, y_grid.astype(BF16)).astype(BF16)

    table[0:n_nodes, :] = nodes[...]
    at = n_nodes
    for source in ((-1, 0), (1, 0), (0, -1), (0, 1)):
        table[at : at + BORDER, :] = slots_in[number(source)][2 * CAP : 2 * CAP + BORDER, :]
        at += BORDER
    table[at:, :] = coarse[...]
    x_edge[:, 0:D] = edges[...]
    x_edge[:, D : 2 * D] = dot_tn(
        down_onehot(table_row(core, edge_sender[...]), table.shape[0]), table[...]
    ).astype(BF16)
    x_edge[:, 2 * D :] = dot_tn(receiver_hot, nodes[...]).astype(BF16)
    y_edge, scale_edge = forward(1, x_edge, slope_edge, hid_edge, norm_edge)
    updated_edges[...] = (edges[...].astype(F32) + y_edge).astype(BF16)
    x_node[:, 2 * D :] = dot(receiver_hot, y_edge.astype(BF16)).astype(BF16)

    y_node, scale_node = forward(2, x_node, slope_node, hid_node, norm_node)
    updated_mesh[...] = (nodes[...].astype(F32) + y_node).astype(BF16)

    d_pre, d_out = backward(2, mesh_cot[...].astype(F32), scale_node, slope_node, norm_node)
    weight_grads(2, x_node, hid_node, d_pre, d_out)
    d_grid = dot_nt(d_pre, w_first[2, D : 2 * D, :]).astype(BF16)
    d_edge = dot_nt(d_pre, w_first[2, 2 * D :, :]).astype(BF16)

    dy = edge_cot[...].astype(F32) + dot_tn(receiver_hot, d_edge)
    d_pre, d_out = backward(1, dy, scale_edge, slope_edge, norm_edge)
    weight_grads(1, x_edge, hid_edge, d_pre, d_out)

    dy = dot_tn(owner_hot, d_grid)
    d_pre, d_out = backward(0, dy, scale_grid, slope_grid, norm_grid)
    weight_grads(0, x_grid, hid_grid, d_pre, d_out)


def layer(core, slots_in, *rest):
    def kernel(core, *refs):
        layer_kernel(core, refs[:9], *refs[9:])

    def rows(n):
        return [
            pltpu.VMEM((n, 3 * D), BF16),
            pltpu.VMEM((n, D), F32),
            pltpu.VMEM((n, D), BF16),
            pltpu.VMEM((n, D), F32),
        ]

    groups = list(zip(rows(288), rows(512), rows(256)))
    scratch = [pltpu.VMEM((1024, D), BF16)] + [s for group in groups for s in group]
    chunks = jax.ShapeDtypeStruct((64, 3, 32, 256), BF16)
    vmem = pl.BlockSpec(memory_space=pltpu.VMEM)
    return pl.pallas_call(
        kernel,
        out_shape=[
            jax.ShapeDtypeStruct((256, D), BF16),
            jax.ShapeDtypeStruct((512, D), BF16),
            chunks,
            chunks,
        ],
        in_specs=[pl.BlockSpec(memory_space=pltpu.SMEM)] + [vmem] * (9 + len(rest)),
        out_specs=[vmem] * 4,
        scratch_shapes=scratch,
        name="layer",
        compiler_params=pltpu.CompilerParams(vmem_limit_bytes=60 << 20),
        cost_estimate=pl.CostEstimate(
            flops=7 * 10**9, bytes_accessed=20 << 20, transcendentals=10**6
        ),
    )(core, *slots_in, *rest)


def finish_kernel(core, parts, grad_first, grad_second, total):
    step = pl.program_id(0)

    @pl.when(step == 0)
    def _():
        total[...] = jnp.zeros_like(total)

    part = parts[0].astype(F32)
    for i in range(1, parts.shape[0]):
        part = part + parts[i].astype(F32)
    total[...] += part

    @pl.when(step == pl.num_programs(0) - 1)
    def _():
        odd = core[0] == 1
        a = total[:, :, 0:128]
        b = total[:, :, 128:256]
        for k in range(3):
            ak, bk = a[k], b[k]
            turned = pltpu.roll(jnp.concatenate([ak, bk], axis=1), 64, 1)
            grad_first[k] = jnp.where(odd, turned[:, 0:192], total[k, :, 0:192])
            grad_second[k] = jnp.where(odd, bk[:, 0:64], turned[:, 0:64])


def finish(core, parts):
    return pl.pallas_call(
        finish_kernel,
        out_shape=[
            jax.ShapeDtypeStruct((3, 32, 192), F32),
            jax.ShapeDtypeStruct((3, 32, 64), F32),
        ],
        grid=(8,),
        in_specs=[
            pl.BlockSpec(memory_space=pltpu.SMEM),
            pl.BlockSpec((8, 3, 32, 256), lambda i: (i, 0, 0, 0)),
        ],
        out_specs=[
            pl.BlockSpec((3, 32, 192), lambda i: (0, 0, 0)),
            pl.BlockSpec((3, 32, 64), lambda i: (0, 0, 0)),
        ],
        scratch_shapes=[pltpu.VMEM((3, 32, 256), F32)],
        name="finish",
        compiler_params=pltpu.CompilerParams(dimension_semantics=("arbitrary",)),
    )(core, parts)


def ring(count, by):
    return [(i, (i + by) % count) for i in range(count)]


def all_coarse(own):
    x = own
    for axis in ("y", "x", "z", "c"):
        count = lax.axis_size(axis)
        moved = [x] + [lax.ppermute(x, axis, ring(count, by)) for by in range(1, count)]
        x = jnp.concatenate(moved, axis=0)
    return x


def shards(
    grid_nodes,
    grid_edges,
    grid_sender,
    owner_index,
    mesh_nodes,
    mesh_edges,
    mesh_sender,
    mesh_receiver,
    w_first,
    first_bias,
    w_second,
    norm_gain,
    mesh_cotangent,
    edge_cotangent,
):
    core = jnp.stack([lax.axis_index(axis).astype(jnp.int32) for axis in ("c", "z", "x", "y")])
    lats = lax.axis_size(LAT)
    lons = lax.axis_size(LON)
    out = packets(grid_nodes, grid_edges, grid_sender.reshape(1, -1), mesh_nodes)
    slots_in = [None] * 9
    slots_in[4] = out[4]
    for offset in MOVED:
        o = number(offset)
        slots_in[8 - o] = lax.ppermute(out[o], ALL, neighbour_pairs(offset, lats, lons))
    coarse = all_coarse(mesh_nodes[mesh_nodes.shape[0] - K_COARSE :])
    updated_mesh, updated_edges, keep, send = layer(
        core,
        slots_in,
        coarse,
        owner_index.reshape(1, -1),
        mesh_sender.reshape(1, -1),
        mesh_receiver.reshape(1, -1),
        mesh_nodes,
        mesh_edges,
        w_first,
        first_bias,
        w_second,
        norm_gain,
        mesh_cotangent,
        edge_cotangent,
    )
    other = lax.ppermute(send, "c", [(0, 1), (1, 0)])
    both = (keep.astype(F32) + other.astype(F32)).astype(BF16)
    parts = lax.all_to_all(both, ("z", "x", "y"), 0, 0, tiled=True)
    first, second = finish(core, parts)
    return (updated_mesh, updated_edges, first.transpose(0, 2, 1), second.transpose(0, 2, 1))


def solution(mesh):
    finer = Mesh(mesh.devices.reshape(4, 2, 4, 4), ALL)
    by_device = P(ALL, None)
    index = P(ALL)
    return jax.shard_map(
        shards,
        mesh=finer,
        in_specs=(
            by_device,
            by_device,
            index,
            index,
            by_device,
            by_device,
            index,
            index,
            P(),
            P(),
            P(),
            P(),
            by_device,
            by_device,
        ),
        out_specs=(by_device, by_device, P(None, LAT, LON), P(None, LAT, LON)),
        check_vma=False,
    )
```

```python
import jax
import jax.numpy as jnp
from jax import lax
from jax.experimental import pallas as pl
from jax.experimental.pallas import tpu as pltpu
from jax.sharding import Mesh
from jax.sharding import PartitionSpec as P

D = 512
CAP = 32
BORDER = 64
K_COARSE = 4
EPSILON = 1e-05
ALL = ("z", "c", "x", "y")
LAT = ("z", "c")
LON = ("x", "y")
F32 = jnp.float32
BF16 = jnp.bfloat16


SLOT_ROWS = 2 * CAP
PACKET = 3 * SLOT_ROWS + BORDER


def lon_pairs(by, lats, lons):
    return [
        (lat * lons + lon, lat * lons + (lon + by) % lons)
        for lat in range(lats)
        for lon in range(lons)
    ]


def chip_pairs(lats, lons):
    pairs = []
    for lat in range(1, lats - 1, 2):
        for lon in range(lons):
            lower, upper = lat * lons + lon, (lat + 1) * lons + lon
            pairs += [(lower, upper), (upper, lower)]
    return pairs


def in_hbm(arrays):
    return [pltpu.with_memory_space_constraint(a, pltpu.HBM) for a in arrays]


def dot(a, b):
    return jnp.dot(a, b, preferred_element_type=F32)


def dot_nt(a, b):
    return lax.dot_general(a, b, (((1,), (1,)), ((), ())), preferred_element_type=F32)


def dot_tn(a, b):
    return lax.dot_general(a, b, (((0,), (0,)), ((), ())), preferred_element_type=F32)


def down_onehot(index, count):
    index = index.reshape(1, -1)
    lines = lax.broadcasted_iota(jnp.int32, (count, index.shape[1]), 0)
    return jnp.where(lines == index, 1.0, 0.0).astype(BF16)


def coarse_line(place, row):
    at = row - 512
    device = at >> 2
    chip = ((device >> 5) << 4) + (device & 15)
    other = ((device >> 4) & 1) ^ place[0]
    return jnp.where(at < 0, -2 * K_COARSE, other * 512 + chip * 8 + (at & 3))


def pack_kernel(core, *refs):
    hbm, (east, west, middle, coarse), (picked, sem), local = (
        refs[:4],
        refs[4:8],
        refs[8:10],
        refs[10:],
    )
    loads = [
        pltpu.make_async_copy(source, to, sem.at[i])
        for i, (source, to) in enumerate(zip(hbm, local))
    ]
    for load in loads:
        load.start()
    for load in loads:
        load.wait()
    points, slot_edges, senders, nodes = local
    picked[...] = dot_tn(down_onehot(senders[...], points.shape[0]), points[...]).astype(BF16)
    toward_core = jnp.where(core[0] == 1, 0, 2)
    bands = (1, toward_core, 2 - toward_core)
    for column, out in ((2, east), (0, west), (1, middle)):
        for at, band in enumerate(bands):
            block = pl.multiple_of((band * 3 + column) * CAP, CAP)
            to = at * SLOT_ROWS
            out[to : to + CAP, :] = slot_edges[pl.ds(block, CAP), :]
            out[to + CAP : to + SLOT_ROWS, :] = picked[pl.ds(block, CAP), :]
        out[3 * SLOT_ROWS : PACKET, :] = nodes[0:BORDER, :]
    rows = nodes[nodes.shape[0] - 8 :, :].astype(F32)[8 - K_COARSE :, :]
    halves = jnp.concatenate([rows[:, : D // 2], rows[:, D // 2 :]], axis=0).astype(BF16)
    coarse[...] = jnp.broadcast_to(halves[None], coarse.shape)


def packets(core, points, slot_edges, senders, nodes):
    packet = jax.ShapeDtypeStruct((PACKET, D), BF16)
    vmem = pl.BlockSpec(memory_space=pltpu.VMEM)
    return pl.pallas_call(
        pack_kernel,
        out_shape=[packet] * 3 + [jax.ShapeDtypeStruct((64, 2 * K_COARSE, D // 2), BF16)],
        in_specs=[pl.BlockSpec(memory_space=pltpu.SMEM)]
        + [pl.BlockSpec(memory_space=pltpu.HBM)] * 4,
        out_specs=[vmem] * 4,
        scratch_shapes=[pltpu.VMEM((9 * CAP, D), BF16), pltpu.SemaphoreType.DMA((4,))]
        + [pltpu.VMEM(a.shape, a.dtype) for a in (points, slot_edges, senders, nodes)],
        name="pack",
        compiler_params=pltpu.CompilerParams(vmem_limit_bytes=16 << 20),
        cost_estimate=pl.CostEstimate(
            flops=2 * 288 * 1024 * 512, bytes_accessed=2 << 20, transcendentals=0
        ),
    )(core, *in_hbm((points, slot_edges, senders, nodes)))


def relay_kernel(from_west, from_east, middle, to_core, to_chip):
    for at, out in ((1, to_core), (2, to_chip)):
        rows = slice(at * SLOT_ROWS, (at + 1) * SLOT_ROWS)
        for i, source in enumerate((from_west, middle, from_east)):
            out[i * SLOT_ROWS : (i + 1) * SLOT_ROWS, :] = source[rows, :]
        out[3 * SLOT_ROWS : PACKET, :] = middle[3 * SLOT_ROWS : PACKET, :]


def relay(from_west, from_east, middle):
    vmem = pl.BlockSpec(memory_space=pltpu.VMEM)
    return pl.pallas_call(
        relay_kernel,
        out_shape=[jax.ShapeDtypeStruct((PACKET, D), BF16)] * 2,
        in_specs=[vmem] * 3,
        out_specs=[vmem] * 2,
        name="relay",
        compiler_params=pltpu.CompilerParams(vmem_limit_bytes=16 << 20),
        cost_estimate=pl.CostEstimate(flops=10**6, bytes_accessed=1 << 20, transcendentals=0),
    )(from_west, from_east, middle)


def layer_kernel(
    core,
    from_west,
    from_east,
    middle,
    from_core,
    from_chip,
    coarse_own,
    coarse_other,
    hbm,
    updated_mesh_out,
    updated_edges_out,
    keep,
    send,
    owner,
    edge_sender,
    edge_receiver,
    first_bias,
    norm_gain,
    nodes,
    edges,
    w_first,
    w_second,
    mesh_cot,
    edge_cot,
    updated_mesh,
    updated_edges,
    sem,
    table,
    x_grid,
    x_edge,
    x_node,
    slope_grid,
    slope_edge,
    slope_node,
    hid_grid,
    hid_edge,
    hid_node,
    norm_grid,
    norm_edge,
    norm_node,
):
    small_to = (owner, edge_sender, edge_receiver, first_bias, norm_gain)
    small_loads = [
        pltpu.make_async_copy(source, to, sem.at[10 + i])
        for i, (source, to) in enumerate(zip(hbm, small_to))
    ]
    nodes_in, edges_in, w_first_in, w_second_in, mesh_cot_in, edge_cot_in = hbm[len(small_to) :]
    loads = [
        pltpu.make_async_copy(source, to, sem.at[i])
        for i, (source, to) in enumerate(
            (
                (nodes_in, nodes),
                (w_first_in.at[0], w_first.at[0]),
                (w_second_in, w_second),
                (edges_in, edges),
                (w_first_in.at[1], w_first.at[1]),
                (w_first_in.at[2], w_first.at[2]),
                (mesh_cot_in, mesh_cot),
                (edge_cot_in, edge_cot),
            )
        )
    ]
    for load in small_loads + loads:
        load.start()
    (
        nodes_load,
        first_0_load,
        second_load,
        edges_load,
        first_1_load,
        first_2_load,
        mesh_cot_load,
        edge_cot_load,
    ) = loads
    store_mesh = pltpu.make_async_copy(updated_mesh, updated_mesh_out, sem.at[8])
    store_edges = pltpu.make_async_copy(updated_edges, updated_edges_out, sem.at[9])
    n_nodes = nodes.shape[0]

    def forward(k, x, slope, hid, norm):
        pre = dot(x[...], w_first[k]) + first_bias[k : k + 1, :]
        sig = 0.5 + 0.5 * jnp.tanh(0.5 * pre)
        act = pre * sig
        hid[...] = act.astype(BF16)
        slope[...] = sig + act * (1.0 - sig)
        out = dot(hid[...], w_second[k])
        out = out - jnp.mean(out, axis=1, keepdims=True)
        scale = lax.rsqrt(jnp.mean(out * out, axis=1, keepdims=True) + EPSILON)
        unit = out * scale
        norm[...] = unit
        return unit * norm_gain[k : k + 1, :], scale

    def backward(k, dy, scale, slope, norm):
        unit = norm[...]
        dn = dy * norm_gain[k : k + 1, :]
        mid = jnp.mean(dn, axis=1, keepdims=True)
        along = jnp.mean(dn * unit, axis=1, keepdims=True)
        d_out = (scale * (dn - mid - unit * along)).astype(BF16)
        d_hid = dot_nt(d_out, w_second[k]).astype(BF16)
        d_pre = (d_hid.astype(F32) * slope[...]).astype(BF16)
        return d_pre, d_out

    odd = core[0] == 1
    low = lax.broadcasted_iota(jnp.int32, (D, 128), 1) < 64

    def weight_grads(k, x, hid, d_pre, d_out):
        second = dot_tn(d_out, hid[...])
        for z in range(4):
            first = dot_tn(d_pre, x[:, 384 * z : 384 * (z + 1)])
            turned = pltpu.roll(second[:, 128 * z : 128 * (z + 1)], 64, 1)
            middle = first[:, 128:256]
            even_a, odd_a = first[:, 0:128], first[:, 256:384]
            even_b = jnp.where(low, middle, turned)
            odd_b = jnp.where(low, turned, middle)
            for ref, a, b in (
                (keep, jnp.where(odd, odd_a, even_a), jnp.where(odd, odd_b, even_b)),
                (send, jnp.where(odd, even_a, odd_a), jnp.where(odd, even_b, odd_b)),
            ):
                ref[16 * z : 16 * (z + 1), k, :, 0:128] = a.astype(BF16).reshape(16, 32, 128)
                ref[16 * z : 16 * (z + 1), k, :, 128:256] = b.astype(BF16).reshape(16, 32, 128)

    lower = jnp.where(odd, from_core[...], from_chip[...])
    upper = jnp.where(odd, from_chip[...], from_core[...])
    same = (from_west[0:SLOT_ROWS, :], middle[0:SLOT_ROWS, :], from_east[0:SLOT_ROWS, :])
    for block in range(9):
        rows = slice(block * CAP, (block + 1) * CAP)
        at = block % 3
        if block // 3 == 1:
            packet = same[at]
        else:
            packet = (lower, None, upper)[block // 3][at * SLOT_ROWS : (at + 1) * SLOT_ROWS, :]
        x_grid[rows, 0:D] = packet[0:CAP, :]
        x_grid[rows, D : 2 * D] = packet[CAP:SLOT_ROWS, :]
    for load in small_loads:
        load.wait()
    owner_hot = down_onehot(owner[...], n_nodes)
    receiver_hot = down_onehot(edge_receiver[...], n_nodes)
    nodes_load.wait()
    x_grid[:, 2 * D :] = dot_tn(owner_hot, nodes[...]).astype(BF16)
    first_0_load.wait()
    second_load.wait()
    y_grid, scale_grid = forward(0, x_grid, slope_grid, hid_grid, norm_grid)
    x_node[:, 0:D] = nodes[...]
    x_node[:, D : 2 * D] = dot(owner_hot, y_grid.astype(BF16)).astype(BF16)

    table[0:n_nodes, :] = nodes[...]
    at = n_nodes
    for border in (
        lower[3 * SLOT_ROWS :, :],
        upper[3 * SLOT_ROWS :, :],
        from_west[3 * SLOT_ROWS :, :],
        from_east[3 * SLOT_ROWS :, :],
    ):
        table[at : at + BORDER, :] = border
        at += BORDER
    edges_load.wait()
    x_edge[:, 0:D] = edges[...]
    sender = edge_sender[...]
    near = dot_tn(down_onehot(sender, at), table[...])
    line = coarse_line(core, sender)
    halves = coarse_own.shape[0]
    for half in range(2):
        hot = down_onehot(line + half * K_COARSE, 2 * halves)
        part = dot_tn(hot[:halves], coarse_own[...]) + dot_tn(hot[halves:], coarse_other[...])
        columns = slice(256 * half, 256 * (half + 1))
        x_edge[:, D + 256 * half : D + 256 * (half + 1)] = (near[:, columns] + part).astype(BF16)
    x_edge[:, 2 * D :] = dot_tn(receiver_hot, nodes[...]).astype(BF16)
    first_1_load.wait()
    y_edge, scale_edge = forward(1, x_edge, slope_edge, hid_edge, norm_edge)
    updated_edges[...] = (edges[...].astype(F32) + y_edge).astype(BF16)
    store_edges.start()
    x_node[:, 2 * D :] = dot(receiver_hot, y_edge.astype(BF16)).astype(BF16)

    first_2_load.wait()
    y_node, scale_node = forward(2, x_node, slope_node, hid_node, norm_node)
    updated_mesh[...] = (nodes[...].astype(F32) + y_node).astype(BF16)

    store_mesh.start()
    mesh_cot_load.wait()
    d_pre, d_out = backward(2, mesh_cot[...].astype(F32), scale_node, slope_node, norm_node)
    weight_grads(2, x_node, hid_node, d_pre, d_out)
    d_grid = dot_nt(d_pre, w_first[2, D : 2 * D, :]).astype(BF16)
    d_edge = dot_nt(d_pre, w_first[2, 2 * D :, :]).astype(BF16)

    edge_cot_load.wait()
    dy = edge_cot[...].astype(F32) + dot_tn(receiver_hot, d_edge)
    d_pre, d_out = backward(1, dy, scale_edge, slope_edge, norm_edge)
    weight_grads(1, x_edge, hid_edge, d_pre, d_out)

    dy = dot_tn(owner_hot, d_grid)
    d_pre, d_out = backward(0, dy, scale_grid, slope_grid, norm_grid)
    weight_grads(0, x_grid, hid_grid, d_pre, d_out)
    store_edges.wait()
    store_mesh.wait()


def layer(core, near, large):
    def kernel(core, *refs):
        n = len(near)
        layer_kernel(core, *refs[:n], refs[n : n + len(large)], *refs[n + len(large) :])

    def rows(n):
        return [
            pltpu.VMEM((n, 3 * D), BF16),
            pltpu.VMEM((n, D), F32),
            pltpu.VMEM((n, D), BF16),
            pltpu.VMEM((n, D), F32),
        ]

    groups = list(zip(rows(288), rows(512), rows(256)))
    scratch = [pltpu.VMEM(a.shape, a.dtype) for a in large]
    scratch += [pltpu.VMEM((256, D), BF16), pltpu.VMEM((512, D), BF16)]
    scratch += [pltpu.SemaphoreType.DMA((15,)), pltpu.VMEM((512, D), BF16)]
    scratch += [s for group in groups for s in group]
    chunks = jax.ShapeDtypeStruct((64, 3, 32, 256), BF16)
    vmem = pl.BlockSpec(memory_space=pltpu.VMEM)
    hbm = pl.BlockSpec(memory_space=pltpu.HBM)
    return pl.pallas_call(
        kernel,
        out_shape=[
            jax.ShapeDtypeStruct((256, D), BF16),
            jax.ShapeDtypeStruct((512, D), BF16),
            chunks,
            chunks,
        ],
        in_specs=[pl.BlockSpec(memory_space=pltpu.SMEM)]
        + [vmem] * len(near)
        + [hbm] * len(large),
        out_specs=[hbm, hbm, vmem, vmem],
        scratch_shapes=scratch,
        name="layer",
        compiler_params=pltpu.CompilerParams(vmem_limit_bytes=40 << 20),
        cost_estimate=pl.CostEstimate(
            flops=7 * 10**9, bytes_accessed=20 << 20, transcendentals=10**6
        ),
    )(core, *near, *in_hbm(large))


def finish_kernel(core, parts, grad_first, grad_second):
    odd = core[0] == 1
    for k in range(3):
        for rows in (slice(0, 16), slice(16, 32)):

            def add(i, total):
                for j in range(4):
                    total = total + parts[4 * i + j, k, rows, :].astype(F32)
                return total

            total = lax.fori_loop(0, parts.shape[0] // 4, add, jnp.zeros((16, 256), F32))
            turned = pltpu.roll(total, 64, 1)
            grad_first[k, rows, :] = jnp.where(odd, turned, total)[:, 0:192]
            grad_second[k, rows, :] = jnp.where(odd, total[:, 128:192], turned[:, 0:64])


def finish(core, parts):
    return pl.pallas_call(
        finish_kernel,
        out_shape=[
            jax.ShapeDtypeStruct((3, 32, 192), F32),
            jax.ShapeDtypeStruct((3, 32, 64), F32),
        ],
        in_specs=[
            pl.BlockSpec(memory_space=pltpu.SMEM),
            pl.BlockSpec(memory_space=pltpu.VMEM),
        ],
        out_specs=[pl.BlockSpec(memory_space=pltpu.VMEM)] * 2,
        name="finish",
        compiler_params=pltpu.CompilerParams(vmem_limit_bytes=16 << 20),
    )(core, parts)


def shards(
    grid_nodes,
    grid_edges,
    grid_sender,
    owner_index,
    mesh_nodes,
    mesh_edges,
    mesh_sender,
    mesh_receiver,
    w_first,
    first_bias,
    w_second,
    norm_gain,
    mesh_cotangent,
    edge_cotangent,
):
    core = jnp.stack([lax.axis_index(axis).astype(jnp.int32) for axis in ("c", "z", "x", "y")])
    lats = lax.axis_size(LAT)
    lons = lax.axis_size(LON)
    swap = [(0, 1), (1, 0)]
    east, west, middle, coarse = packets(core, grid_nodes, grid_edges, grid_sender, mesh_nodes)
    from_west = lax.ppermute(east, ALL, lon_pairs(1, lats, lons))
    from_east = lax.ppermute(west, ALL, lon_pairs(-1, lats, lons))
    coarse_own = lax.all_to_all(coarse, ("z", "x", "y"), 0, 0, tiled=True).reshape(-1, D // 2)
    to_core, to_chip = relay(from_west, from_east, middle)
    from_chip = lax.ppermute(to_chip, ALL, chip_pairs(lats, lons))
    from_core = lax.ppermute(to_core, "c", swap)
    coarse_other = lax.ppermute(coarse_own, "c", swap)
    updated_mesh, updated_edges, keep, send = layer(
        core,
        (from_west, from_east, middle, from_core, from_chip, coarse_own, coarse_other),
        (
            owner_index,
            mesh_sender,
            mesh_receiver,
            first_bias,
            norm_gain,
            mesh_nodes,
            mesh_edges,
            w_first,
            w_second,
            mesh_cotangent,
            edge_cotangent,
        ),
    )
    other = lax.ppermute(send, "c", swap)
    both = (keep.astype(F32) + other.astype(F32)).astype(BF16)
    parts = lax.all_to_all(both, ("z", "x", "y"), 0, 0, tiled=True)
    first, second = finish(core, parts)
    return (updated_mesh, updated_edges, first.transpose(0, 2, 1), second.transpose(0, 2, 1))


def solution(mesh):
    finer = Mesh(mesh.devices.reshape(4, 2, 4, 4), ALL)
    by_device = P(ALL, None)
    index = P(ALL)
    return jax.shard_map(
        shards,
        mesh=finer,
        in_specs=(
            by_device,
            by_device,
            index,
            index,
            by_device,
            by_device,
            index,
            index,
            P(),
            P(),
            P(),
            P(),
            by_device,
            by_device,
        ),
        out_specs=(by_device, by_device, P(None, LAT, LON), P(None, LAT, LON)),
        check_vma=False,
    )
```

```python
import jax
import jax.numpy as jnp
from jax import lax
from jax.experimental import pallas as pl
from jax.experimental.pallas import tpu as pltpu
from jax.sharding import Mesh
from jax.sharding import PartitionSpec as P

D = 512
CAP = 32
BORDER = 64
K_COARSE = 4
EPSILON = 1e-05
ALL = ("z", "c", "x", "y")
LAT = ("z", "c")
LON = ("x", "y")
F32 = jnp.float32
BF16 = jnp.bfloat16


SLOT_ROWS = 2 * CAP
PACKET = 3 * SLOT_ROWS + BORDER


def lon_pairs(by, lats, lons):
    return [
        (lat * lons + lon, lat * lons + (lon + by) % lons)
        for lat in range(lats)
        for lon in range(lons)
    ]


def chip_pairs(lats, lons):
    pairs = []
    for lat in range(1, lats - 1, 2):
        for lon in range(lons):
            lower, upper = lat * lons + lon, (lat + 1) * lons + lon
            pairs += [(lower, upper), (upper, lower)]
    return pairs


def in_hbm(arrays):
    return [pltpu.with_memory_space_constraint(a, pltpu.HBM) for a in arrays]


def dot(a, b):
    return jnp.dot(a, b, preferred_element_type=F32)


def dot_nt(a, b):
    return lax.dot_general(a, b, (((1,), (1,)), ((), ())), preferred_element_type=F32)


def dot_tn(a, b):
    return lax.dot_general(a, b, (((0,), (0,)), ((), ())), preferred_element_type=F32)


def down_onehot(index, count):
    index = index.reshape(1, -1)
    lines = lax.broadcasted_iota(jnp.int32, (count, index.shape[1]), 0)
    return jnp.where(lines == index, 1.0, 0.0).astype(BF16)


def coarse_line(row):
    at = row - 512
    device = at >> 2
    chip = ((device >> 5) << 4) + (device & 15)
    other = ((device >> 4) & 1) ^ lax.axis_index("c")
    return jnp.where(at < 0, -2 * K_COARSE, other * 512 + chip * 8 + (at & 3))


def pack_kernel(*refs):
    hbm, (east, west, middle, coarse), (picked, sem), local = (
        refs[:4],
        refs[4:8],
        refs[8:10],
        refs[10:],
    )
    loads = [
        pltpu.make_async_copy(source, to, sem.at[i])
        for i, (source, to) in enumerate(zip(hbm, local))
    ]
    for load in loads:
        load.start()
    for load in loads:
        load.wait()
    points, slot_edges, senders, nodes = local
    picked[...] = dot_tn(down_onehot(senders[...], points.shape[0]), points[...]).astype(BF16)
    toward_core = jnp.where(lax.axis_index("c") == 1, 0, 2)
    bands = (1, toward_core, 2 - toward_core)
    for column, out in ((2, east), (0, west), (1, middle)):
        for at, band in enumerate(bands):
            block = pl.multiple_of((band * 3 + column) * CAP, CAP)
            to = at * SLOT_ROWS
            out[to : to + CAP, :] = slot_edges[pl.ds(block, CAP), :]
            out[to + CAP : to + SLOT_ROWS, :] = picked[pl.ds(block, CAP), :]
        out[3 * SLOT_ROWS : PACKET, :] = nodes[0:BORDER, :]
    rows = nodes[nodes.shape[0] - 8 :, :].astype(F32)[8 - K_COARSE :, :]
    halves = jnp.concatenate([rows[:, : D // 2], rows[:, D // 2 :]], axis=0).astype(BF16)
    coarse[...] = jnp.broadcast_to(halves[None], coarse.shape)


def packets(points, slot_edges, senders, nodes):
    packet = jax.ShapeDtypeStruct((PACKET, D), BF16)
    vmem = pl.BlockSpec(memory_space=pltpu.VMEM)
    return pl.pallas_call(
        pack_kernel,
        out_shape=[packet] * 3 + [jax.ShapeDtypeStruct((64, 2 * K_COARSE, D // 2), BF16)],
        in_specs=[pl.BlockSpec(memory_space=pltpu.HBM)] * 4,
        out_specs=[vmem] * 4,
        scratch_shapes=[pltpu.VMEM((9 * CAP, D), BF16), pltpu.SemaphoreType.DMA((4,))]
        + [pltpu.VMEM(a.shape, a.dtype) for a in (points, slot_edges, senders, nodes)],
        name="pack",
        compiler_params=pltpu.CompilerParams(vmem_limit_bytes=16 << 20),
        cost_estimate=pl.CostEstimate(
            flops=2 * 288 * 1024 * 512, bytes_accessed=2 << 20, transcendentals=0
        ),
    )(*in_hbm((points, slot_edges, senders, nodes)))


def relay_kernel(from_west, from_east, middle, to_core, to_chip):
    for at, out in ((1, to_core), (2, to_chip)):
        rows = slice(at * SLOT_ROWS, (at + 1) * SLOT_ROWS)
        for i, source in enumerate((from_west, middle, from_east)):
            out[i * SLOT_ROWS : (i + 1) * SLOT_ROWS, :] = source[rows, :]
        out[3 * SLOT_ROWS : PACKET, :] = middle[3 * SLOT_ROWS : PACKET, :]


def relay(from_west, from_east, middle):
    vmem = pl.BlockSpec(memory_space=pltpu.VMEM)
    return pl.pallas_call(
        relay_kernel,
        out_shape=[jax.ShapeDtypeStruct((PACKET, D), BF16)] * 2,
        in_specs=[vmem] * 3,
        out_specs=[vmem] * 2,
        name="relay",
        compiler_params=pltpu.CompilerParams(vmem_limit_bytes=16 << 20),
        cost_estimate=pl.CostEstimate(flops=10**6, bytes_accessed=1 << 20, transcendentals=0),
    )(from_west, from_east, middle)


def layer_kernel(
    from_west,
    from_east,
    middle,
    from_core,
    from_chip,
    coarse_own,
    coarse_other,
    hbm,
    updated_mesh_out,
    updated_edges_out,
    keep_0,
    keep_1,
    keep_2,
    send_0,
    send_1,
    send_2,
    owner,
    edge_sender,
    edge_receiver,
    first_bias,
    norm_gain,
    nodes,
    edges,
    w_first,
    w_second,
    mesh_cot,
    edge_cot,
    updated_mesh,
    updated_edges,
    sem,
    table,
    x_grid,
    x_edge,
    x_node,
    slope_grid,
    slope_edge,
    slope_node,
    hid_grid,
    hid_edge,
    hid_node,
    norm_grid,
    norm_edge,
    norm_node,
):
    small_to = (owner, edge_sender, edge_receiver, first_bias, norm_gain)
    small_loads = [
        pltpu.make_async_copy(source, to, sem.at[10 + i])
        for i, (source, to) in enumerate(zip(hbm, small_to))
    ]
    nodes_in, edges_in, w_first_in, w_second_in, mesh_cot_in, edge_cot_in = hbm[len(small_to) :]
    loads = [
        pltpu.make_async_copy(source, to, sem.at[i])
        for i, (source, to) in enumerate(
            (
                (nodes_in, nodes),
                (w_first_in.at[0], w_first.at[0]),
                (w_second_in, w_second),
                (edges_in, edges),
                (w_first_in.at[1], w_first.at[1]),
                (w_first_in.at[2], w_first.at[2]),
                (mesh_cot_in, mesh_cot),
                (edge_cot_in, edge_cot),
            )
        )
    ]
    for load in small_loads + loads:
        load.start()
    (
        nodes_load,
        first_0_load,
        second_load,
        edges_load,
        first_1_load,
        first_2_load,
        mesh_cot_load,
        edge_cot_load,
    ) = loads
    store_mesh = pltpu.make_async_copy(updated_mesh, updated_mesh_out, sem.at[8])
    store_edges = pltpu.make_async_copy(updated_edges, updated_edges_out, sem.at[9])
    n_nodes = nodes.shape[0]

    def forward(k, x, slope, hid, norm):
        pre = dot(x[...], w_first[k]) + first_bias[k : k + 1, :]
        sig = 0.5 + 0.5 * jnp.tanh(0.5 * pre)
        act = pre * sig
        hid[...] = act.astype(BF16)
        slope[...] = sig + act * (1.0 - sig)
        out = dot(hid[...], w_second[k])
        out = out - jnp.mean(out, axis=1, keepdims=True)
        scale = lax.rsqrt(jnp.mean(out * out, axis=1, keepdims=True) + EPSILON)
        unit = out * scale
        norm[...] = unit
        return unit * norm_gain[k : k + 1, :], scale

    def backward(k, dy, scale, slope, norm):
        unit = norm[...]
        dn = dy * norm_gain[k : k + 1, :]
        mid = jnp.mean(dn, axis=1, keepdims=True)
        along = jnp.mean(dn * unit, axis=1, keepdims=True)
        d_out = (scale * (dn - mid - unit * along)).astype(BF16)
        d_hid = dot_nt(d_out, w_second[k]).astype(BF16)
        d_pre = (d_hid.astype(F32) * slope[...]).astype(BF16)
        return d_pre, d_out

    odd = lax.axis_index("c") == 1
    low = lax.broadcasted_iota(jnp.int32, (D, 128), 1) < 64

    def weight_grads(k, x, hid, d_pre, d_out):
        second = dot_tn(d_out, hid[...])
        for z in range(4):
            first = dot_tn(d_pre, x[:, 384 * z : 384 * (z + 1)])
            turned = pltpu.roll(second[:, 128 * z : 128 * (z + 1)], 64, 1)
            middle = first[:, 128:256]
            even_a, odd_a = first[:, 0:128], first[:, 256:384]
            even_b = jnp.where(low, middle, turned)
            odd_b = jnp.where(low, turned, middle)
            keep, send = (keep_0, keep_1, keep_2)[k], (send_0, send_1, send_2)[k]
            for ref, a, b in (
                (keep, jnp.where(odd, odd_a, even_a), jnp.where(odd, odd_b, even_b)),
                (send, jnp.where(odd, even_a, odd_a), jnp.where(odd, even_b, odd_b)),
            ):
                ref[16 * z : 16 * (z + 1), :, 0:128] = a.astype(BF16).reshape(16, 32, 128)
                ref[16 * z : 16 * (z + 1), :, 128:256] = b.astype(BF16).reshape(16, 32, 128)

    lower = jnp.where(odd, from_core[...], from_chip[...])
    upper = jnp.where(odd, from_chip[...], from_core[...])
    same = (from_west[0:SLOT_ROWS, :], middle[0:SLOT_ROWS, :], from_east[0:SLOT_ROWS, :])
    for block in range(9):
        rows = slice(block * CAP, (block + 1) * CAP)
        at = block % 3
        if block // 3 == 1:
            packet = same[at]
        else:
            packet = (lower, None, upper)[block // 3][at * SLOT_ROWS : (at + 1) * SLOT_ROWS, :]
        x_grid[rows, 0:D] = packet[0:CAP, :]
        x_grid[rows, D : 2 * D] = packet[CAP:SLOT_ROWS, :]
    for load in small_loads:
        load.wait()
    owner_hot = down_onehot(owner[...], n_nodes)
    receiver_hot = down_onehot(edge_receiver[...], n_nodes)
    nodes_load.wait()
    x_grid[:, 2 * D :] = dot_tn(owner_hot, nodes[...]).astype(BF16)
    first_0_load.wait()
    second_load.wait()
    y_grid, scale_grid = forward(0, x_grid, slope_grid, hid_grid, norm_grid)
    x_node[:, 0:D] = nodes[...]
    x_node[:, D : 2 * D] = dot(owner_hot, y_grid.astype(BF16)).astype(BF16)

    table[0:n_nodes, :] = nodes[...]
    at = n_nodes
    for border in (
        lower[3 * SLOT_ROWS :, :],
        upper[3 * SLOT_ROWS :, :],
        from_west[3 * SLOT_ROWS :, :],
        from_east[3 * SLOT_ROWS :, :],
    ):
        table[at : at + BORDER, :] = border
        at += BORDER
    edges_load.wait()
    x_edge[:, 0:D] = edges[...]
    sender = edge_sender[...]
    near = dot_tn(down_onehot(sender, at), table[...])
    line = coarse_line(sender)
    halves = coarse_own.shape[0]
    for half in range(2):
        hot = down_onehot(line + half * K_COARSE, 2 * halves)
        part = dot_tn(hot[:halves], coarse_own[...]) + dot_tn(hot[halves:], coarse_other[...])
        columns = slice(256 * half, 256 * (half + 1))
        x_edge[:, D + 256 * half : D + 256 * (half + 1)] = (near[:, columns] + part).astype(BF16)
    x_edge[:, 2 * D :] = dot_tn(receiver_hot, nodes[...]).astype(BF16)
    first_1_load.wait()
    y_edge, scale_edge = forward(1, x_edge, slope_edge, hid_edge, norm_edge)
    updated_edges[...] = (edges[...].astype(F32) + y_edge).astype(BF16)
    store_edges.start()
    x_node[:, 2 * D :] = dot(receiver_hot, y_edge.astype(BF16)).astype(BF16)

    first_2_load.wait()
    y_node, scale_node = forward(2, x_node, slope_node, hid_node, norm_node)
    updated_mesh[...] = (nodes[...].astype(F32) + y_node).astype(BF16)

    store_mesh.start()
    mesh_cot_load.wait()
    d_pre, d_out = backward(2, mesh_cot[...].astype(F32), scale_node, slope_node, norm_node)
    weight_grads(2, x_node, hid_node, d_pre, d_out)
    d_grid = dot_nt(d_pre, w_first[2, D : 2 * D, :]).astype(BF16)
    d_edge = dot_nt(d_pre, w_first[2, 2 * D :, :]).astype(BF16)

    edge_cot_load.wait()
    dy = edge_cot[...].astype(F32) + dot_tn(receiver_hot, d_edge)
    d_pre, d_out = backward(1, dy, scale_edge, slope_edge, norm_edge)
    weight_grads(1, x_edge, hid_edge, d_pre, d_out)

    dy = dot_tn(owner_hot, d_grid)
    d_pre, d_out = backward(0, dy, scale_grid, slope_grid, norm_grid)
    weight_grads(0, x_grid, hid_grid, d_pre, d_out)
    store_edges.wait()
    store_mesh.wait()


def layer(near, large):
    def kernel(*refs):
        n = len(near)
        layer_kernel(*refs[:n], refs[n : n + len(large)], *refs[n + len(large) :])

    def rows(n):
        return [
            pltpu.VMEM((n, 3 * D), BF16),
            pltpu.VMEM((n, D), F32),
            pltpu.VMEM((n, D), BF16),
            pltpu.VMEM((n, D), F32),
        ]

    groups = list(zip(rows(288), rows(512), rows(256)))
    scratch = [pltpu.VMEM(a.shape, a.dtype) for a in large]
    scratch += [pltpu.VMEM((256, D), BF16), pltpu.VMEM((512, D), BF16)]
    scratch += [pltpu.SemaphoreType.DMA((15,)), pltpu.VMEM((512, D), BF16)]
    scratch += [s for group in groups for s in group]
    chunks = jax.ShapeDtypeStruct((64, 32, 256), BF16)
    vmem = pl.BlockSpec(memory_space=pltpu.VMEM)
    hbm = pl.BlockSpec(memory_space=pltpu.HBM)
    return pl.pallas_call(
        kernel,
        out_shape=[
            jax.ShapeDtypeStruct((256, D), BF16),
            jax.ShapeDtypeStruct((512, D), BF16),
        ]
        + [chunks] * 6,
        in_specs=[vmem] * len(near) + [hbm] * len(large),
        out_specs=[hbm, hbm] + [vmem] * 6,
        scratch_shapes=scratch,
        name="layer",
        compiler_params=pltpu.CompilerParams(vmem_limit_bytes=40 << 20),
        cost_estimate=pl.CostEstimate(
            flops=7 * 10**9, bytes_accessed=20 << 20, transcendentals=10**6
        ),
    )(*near, *in_hbm(large))


def this_place():
    return [lax.axis_index(axis) for axis in ("c", "z", "x", "y")]


def small_call(kernel, name, shapes, *args):
    vmem = pl.BlockSpec(memory_space=pltpu.VMEM)
    moved = sum(a.size * 2 for a in args)
    return pl.pallas_call(
        kernel,
        out_shape=[jax.ShapeDtypeStruct(shape, dtype) for shape, dtype in shapes],
        in_specs=[vmem] * len(args),
        out_specs=[vmem] * len(shapes),
        name=name,
        compiler_params=pltpu.CompilerParams(vmem_limit_bytes=12 << 20),
        cost_estimate=pl.CostEstimate(flops=moved, bytes_accessed=moved, transcendentals=0),
    )(*args)


Z, X, Y = 1, 2, 3
AXES = {0: (Y, X, Z), 1: (X, Z, Y), 2: (Z, Y, X)}


def masks(place):
    return 1 + 2 * place[0], 3 - 2 * place[0]


def partner_pairs(axis, second):
    pairs = []
    for device in range(128):
        z, c, x, y = device >> 5, (device >> 4) & 1, (device >> 2) & 3, device & 3
        mask = (3 - 2 * c) if second else (1 + 2 * c)
        at = {Z: z, X: x, Y: y}
        at[axis] ^= mask
        pairs.append((device, ((at[Z] * 2 + c) * 4 + at[X]) * 4 + at[Y]))
    return pairs


def swap_along(value, axis, second):
    return lax.ppermute(value, ALL, partner_pairs(axis, second))


def chunk_at(left, axis, i, r):
    n = len(left)
    stride = 4 ** (n - 1 - left.index(axis))
    low = r & (stride - 1)
    return (r - low) * 4 + i * stride + low


def halve(k, step, *inputs):
    axis = AXES[k][step]
    left = sorted(AXES[k][step:])
    count = 4 ** (len(left) - 1)

    def kernel(a, b, kept, sent):
        place = this_place()
        m1, m2 = masks(place)
        mine = place[axis]
        for out, base in ((kept, mine), (sent, mine ^ m1)):
            for j in range(2):
                i = base ^ (m2 * j)

                def body(r, carry):
                    at = chunk_at(left, axis, i, r)
                    out[j, r] = a[at] + b[at]
                    return carry

                lax.fori_loop(0, count, body, 0, unroll=min(count, 8))

    half = ((2, count, 32, 256), BF16)
    return small_call(kernel, f"halve_{k}_{step}", (half, half), *inputs)


def quarter(k, step, kept, got):
    count = kept.shape[1]

    def kernel(kept, got, keep, send):
        for j, out in ((0, keep), (1, send)):

            def body(r, carry):
                out[r] = kept[j, r] + got[j, r]
                return carry

            lax.fori_loop(0, count, body, 0, unroll=min(count, 8))

    half = ((count, 32, 256), BF16)
    return small_call(kernel, f"quarter_{k}_{step}", (half, half), kept, got)


def reduced(k, keep, got):
    for step, axis in enumerate(AXES[k]):
        keep, send = halve(k, step, keep, got)
        keep, send = quarter(k, step, keep, swap_along(send, axis, False))
        got = swap_along(send, axis, True)
    return keep, got


def finish(terms):
    def kernel(*refs):
        grad_first, grad_second = refs[6:]
        odd = lax.axis_index("c") == 1
        for k in range(3):
            total = refs[2 * k][0].astype(F32) + refs[2 * k + 1][0].astype(F32)
            turned = pltpu.roll(total, 64, 1)
            grad_first[k] = jnp.where(odd, turned, total)[:, 0:192]
            grad_second[k] = jnp.where(odd, total[:, 128:192], turned[:, 0:64])

    shapes = (((3, 32, 192), F32), ((3, 32, 64), F32))
    return small_call(kernel, "finish", shapes, *[t for pair in terms for t in pair])


def shards(
    grid_nodes,
    grid_edges,
    grid_sender,
    owner_index,
    mesh_nodes,
    mesh_edges,
    mesh_sender,
    mesh_receiver,
    w_first,
    first_bias,
    w_second,
    norm_gain,
    mesh_cotangent,
    edge_cotangent,
):
    lats = lax.axis_size(LAT)
    lons = lax.axis_size(LON)
    swap = [(0, 1), (1, 0)]
    east, west, middle, coarse = packets(grid_nodes, grid_edges, grid_sender, mesh_nodes)
    from_west = lax.ppermute(east, ALL, lon_pairs(1, lats, lons))
    from_east = lax.ppermute(west, ALL, lon_pairs(-1, lats, lons))
    coarse_own = lax.all_to_all(coarse, ("z", "x", "y"), 0, 0, tiled=True).reshape(-1, D // 2)
    to_core, to_chip = relay(from_west, from_east, middle)
    from_chip = lax.ppermute(to_chip, ALL, chip_pairs(lats, lons))
    from_core = lax.ppermute(to_core, "c", swap)
    coarse_other = lax.ppermute(coarse_own, "c", swap)
    updated_mesh, updated_edges, *parts = layer(
        (from_west, from_east, middle, from_core, from_chip, coarse_own, coarse_other),
        (
            owner_index,
            mesh_sender,
            mesh_receiver,
            first_bias,
            norm_gain,
            mesh_nodes,
            mesh_edges,
            w_first,
            w_second,
            mesh_cotangent,
            edge_cotangent,
        ),
    )
    terms = {}
    for k in (2, 1, 0):
        terms[k] = reduced(k, parts[k], lax.ppermute(parts[3 + k], "c", swap))
    first, second = finish([terms[k] for k in range(3)])
    return (updated_mesh, updated_edges, first.transpose(0, 2, 1), second.transpose(0, 2, 1))


def solution(mesh):
    finer = Mesh(mesh.devices.reshape(4, 2, 4, 4), ALL)
    by_device = P(ALL, None)
    index = P(ALL)
    return jax.shard_map(
        shards,
        mesh=finer,
        in_specs=(
            by_device,
            by_device,
            index,
            index,
            by_device,
            by_device,
            index,
            index,
            P(),
            P(),
            P(),
            P(),
            by_device,
            by_device,
        ),
        out_specs=(by_device, by_device, P(None, LAT, LON), P(None, LAT, LON)),
        check_vma=False,
    )
```

```python
import jax
import jax.numpy as jnp
from jax import lax
from jax.experimental import pallas as pl
from jax.experimental.pallas import tpu as pltpu
from jax.sharding import Mesh
from jax.sharding import PartitionSpec as P

D = 512
CAP = 32
BORDER = 64
K_COARSE = 4
EPSILON = 1e-05
ALL = ("z", "c", "x", "y")
LAT = ("z", "c")
LON = ("x", "y")
F32 = jnp.float32
BF16 = jnp.bfloat16


SLOT_ROWS = 2 * CAP
PACKET = 3 * SLOT_ROWS + BORDER


def lon_pairs(by, lats, lons):
    return [
        (lat * lons + lon, lat * lons + (lon + by) % lons)
        for lat in range(lats)
        for lon in range(lons)
    ]


def chip_pairs(lats, lons):
    pairs = []
    for lat in range(1, lats - 1, 2):
        for lon in range(lons):
            lower, upper = lat * lons + lon, (lat + 1) * lons + lon
            pairs += [(lower, upper), (upper, lower)]
    return pairs


def in_hbm(arrays):
    return [pltpu.with_memory_space_constraint(a, pltpu.HBM) for a in arrays]


def dot(a, b):
    return jnp.dot(a, b, preferred_element_type=F32)


def dot_nt(a, b):
    return lax.dot_general(a, b, (((1,), (1,)), ((), ())), preferred_element_type=F32)


def dot_tn(a, b):
    return lax.dot_general(a, b, (((0,), (0,)), ((), ())), preferred_element_type=F32)


def down_onehot(index, count):
    index = index.reshape(1, -1)
    lines = lax.broadcasted_iota(jnp.int32, (count, index.shape[1]), 0)
    return jnp.where(lines == index, 1.0, 0.0).astype(BF16)


def coarse_line(row):
    at = row - 512
    device = at >> 2
    chip = ((device >> 5) << 4) + (device & 15)
    other = ((device >> 4) & 1) ^ lax.axis_index("c")
    return jnp.where(at < 0, -2 * K_COARSE, other * 512 + chip * 8 + (at & 3))


def pack_kernel(*refs):
    hbm, (east, west, middle, coarse), (picked, sem), local = (
        refs[:4],
        refs[4:8],
        refs[8:10],
        refs[10:],
    )
    loads = [
        pltpu.make_async_copy(source, to, sem.at[i])
        for i, (source, to) in enumerate(zip(hbm, local))
    ]
    for load in loads:
        load.start()
    for load in loads:
        load.wait()
    points, slot_edges, senders, nodes = local
    picked[...] = dot_tn(down_onehot(senders[...], points.shape[0]), points[...]).astype(BF16)
    toward_core = jnp.where(lax.axis_index("c") == 1, 0, 2)
    bands = (1, toward_core, 2 - toward_core)
    for column, out in ((2, east), (0, west), (1, middle)):
        for at, band in enumerate(bands):
            block = pl.multiple_of((band * 3 + column) * CAP, CAP)
            to = at * SLOT_ROWS
            out[to : to + CAP, :] = slot_edges[pl.ds(block, CAP), :]
            out[to + CAP : to + SLOT_ROWS, :] = picked[pl.ds(block, CAP), :]
        out[3 * SLOT_ROWS : PACKET, :] = nodes[0:BORDER, :]
    rows = nodes[nodes.shape[0] - 8 :, :].astype(F32)[8 - K_COARSE :, :]
    halves = jnp.concatenate([rows[:, : D // 2], rows[:, D // 2 :]], axis=0).astype(BF16)
    coarse[...] = jnp.broadcast_to(halves[None], coarse.shape)


def packets(points, slot_edges, senders, nodes):
    packet = jax.ShapeDtypeStruct((PACKET, D), BF16)
    vmem = pl.BlockSpec(memory_space=pltpu.VMEM)
    return pl.pallas_call(
        pack_kernel,
        out_shape=[packet] * 3 + [jax.ShapeDtypeStruct((64, 2 * K_COARSE, D // 2), BF16)],
        in_specs=[pl.BlockSpec(memory_space=pltpu.HBM)] * 4,
        out_specs=[vmem] * 4,
        scratch_shapes=[pltpu.VMEM((9 * CAP, D), BF16), pltpu.SemaphoreType.DMA((4,))]
        + [pltpu.VMEM(a.shape, a.dtype) for a in (points, slot_edges, senders, nodes)],
        name="pack",
        compiler_params=pltpu.CompilerParams(vmem_limit_bytes=16 << 20),
        cost_estimate=pl.CostEstimate(
            flops=2 * 288 * 1024 * 512, bytes_accessed=2 << 20, transcendentals=0
        ),
    )(*in_hbm((points, slot_edges, senders, nodes)))


def relay_kernel(from_west, from_east, middle, to_core, to_chip):
    for at, out in ((1, to_core), (2, to_chip)):
        rows = slice(at * SLOT_ROWS, (at + 1) * SLOT_ROWS)
        for i, source in enumerate((from_west, middle, from_east)):
            out[i * SLOT_ROWS : (i + 1) * SLOT_ROWS, :] = source[rows, :]
        out[3 * SLOT_ROWS : PACKET, :] = middle[3 * SLOT_ROWS : PACKET, :]


def relay(from_west, from_east, middle):
    vmem = pl.BlockSpec(memory_space=pltpu.VMEM)
    return pl.pallas_call(
        relay_kernel,
        out_shape=[jax.ShapeDtypeStruct((PACKET, D), BF16)] * 2,
        in_specs=[vmem] * 3,
        out_specs=[vmem] * 2,
        name="relay",
        compiler_params=pltpu.CompilerParams(vmem_limit_bytes=16 << 20),
        cost_estimate=pl.CostEstimate(flops=10**6, bytes_accessed=1 << 20, transcendentals=0),
    )(from_west, from_east, middle)


def forward(pre, w_second, gain, slope, hid, norm, scale):
    sig = 0.5 + 0.5 * jnp.tanh(0.5 * pre)
    act = pre * sig
    hid[...] = act.astype(BF16)
    slope[...] = sig + act * (1.0 - sig)
    out = dot(hid[...], w_second)
    out = out - jnp.mean(out, axis=1, keepdims=True)
    size = lax.rsqrt(jnp.mean(out * out, axis=1, keepdims=True) + EPSILON)
    scale[...] = jnp.broadcast_to(size, scale.shape)
    unit = out * size
    norm[...] = unit
    return unit * gain


def backward(dy, w_second, gain, slope, norm, scale):
    unit = norm[...]
    dn = dy * gain
    mid = jnp.mean(dn, axis=1, keepdims=True)
    along = jnp.mean(dn * unit, axis=1, keepdims=True)
    d_out = (scale[:, 0:1] * (dn - mid - unit * along)).astype(BF16)
    d_hid = dot_nt(d_out, w_second).astype(BF16)
    d_pre = (d_hid.astype(F32) * slope[...]).astype(BF16)
    return d_pre, d_out


def weight_grads(x, hid, d_pre, d_out, keep, send):
    odd = lax.axis_index("c") == 1
    low = lax.broadcasted_iota(jnp.int32, (D, 128), 1) < 64
    second = dot_tn(d_out, hid[...])
    for z in range(4):
        first = dot_tn(d_pre, x[:, 384 * z : 384 * (z + 1)])
        turned = pltpu.roll(second[:, 128 * z : 128 * (z + 1)], 64, 1)
        middle = first[:, 128:256]
        even_a, odd_a = first[:, 0:128], first[:, 256:384]
        even_b = jnp.where(low, middle, turned)
        odd_b = jnp.where(low, turned, middle)
        for ref, a, b in (
            (keep, jnp.where(odd, odd_a, even_a), jnp.where(odd, odd_b, even_b)),
            (send, jnp.where(odd, even_a, odd_a), jnp.where(odd, even_b, odd_b)),
        ):
            ref[16 * z : 16 * (z + 1), :, 0:128] = a.astype(BF16).reshape(16, 32, 128)
            ref[16 * z : 16 * (z + 1), :, 128:256] = b.astype(BF16).reshape(16, 32, 128)


LOADED = (
    "edge_receiver",
    "mesh_sender",
    "nodes",
    "w_first",
    "edges",
    "first_bias",
    "owner",
    "norm_gain",
    "w_second",
    "mesh_cot",
    "edge_cot",
)


def local_kernel(from_west, from_east, coarse_own, coarse_other, *refs):
    n = len(LOADED)
    hbm, vmem = refs[:n], refs[n : 2 * n]
    middle, received, pre, sem, table = refs[2 * n :]
    to = dict(zip(LOADED, vmem))
    loads = {
        name: pltpu.make_async_copy(source, target, sem.at[i])
        for i, (name, source, target) in enumerate(zip(LOADED, hbm, vmem))
        if name != "w_first"
    }
    w_first = dict(zip(LOADED, hbm))["w_first"]
    for k in range(3):
        loads[f"w_first_{k}"] = pltpu.make_async_copy(
            w_first.at[k], to["w_first"].at[k], sem.at[n + k]
        )
    for name in ("edge_receiver", "mesh_sender", "nodes", "w_first_1", "edges", "first_bias"):
        loads[name].start()
    rest = [name for name in loads if name in ("owner", "norm_gain", "w_second", "mesh_cot", "edge_cot")]
    rest += ["w_first_0", "w_first_2"]
    for name in rest:
        loads[name].start()
    for name in ("edge_receiver", "mesh_sender", "nodes"):
        loads[name].wait()
    nodes = to["nodes"]
    n_nodes = nodes.shape[0]
    table[0:n_nodes, :] = nodes[...]
    table[n_nodes : n_nodes + BORDER, :] = from_west[3 * SLOT_ROWS :, :]
    table[n_nodes + BORDER :, :] = from_east[3 * SLOT_ROWS :, :]
    sender = to["mesh_sender"][...]
    line = jnp.where(sender < n_nodes, sender, jnp.where(sender < n_nodes + 2 * BORDER, -1, sender - 2 * BORDER))
    near = dot_tn(down_onehot(line, table.shape[0]), table[...])
    line = coarse_line(sender)
    halves = coarse_own.shape[0]
    for half in range(2):
        hot = down_onehot(line + half * K_COARSE, 2 * halves)
        part = dot_tn(hot[:halves], coarse_own[...]) + dot_tn(hot[halves:], coarse_other[...])
        columns = slice(256 * half, 256 * (half + 1))
        middle[:, columns] = (near[:, columns] + part).astype(BF16)
    received[...] = dot_tn(down_onehot(to["edge_receiver"][...], n_nodes), nodes[...]).astype(BF16)
    for name in ("w_first_1", "edges", "first_bias"):
        loads[name].wait()
    w = to["w_first"]
    pre[...] = (
        dot(to["edges"][...], w[1, 0:D, :])
        + dot(received[...], w[1, 2 * D :, :])
        + to["first_bias"][1:2, :]
    )
    for name in rest:
        loads[name].wait()


def local(near, loaded):
    vmem = pl.BlockSpec(memory_space=pltpu.VMEM)
    hbm = pl.BlockSpec(memory_space=pltpu.HBM)
    out = pl.pallas_call(
        local_kernel,
        out_shape=[jax.ShapeDtypeStruct(a.shape, a.dtype) for a in loaded]
        + [
            jax.ShapeDtypeStruct((512, D), BF16),
            jax.ShapeDtypeStruct((512, D), BF16),
            jax.ShapeDtypeStruct((512, D), F32),
        ],
        in_specs=[vmem] * len(near) + [hbm] * len(loaded),
        out_specs=[vmem] * (len(loaded) + 3),
        scratch_shapes=[
            pltpu.SemaphoreType.DMA((len(loaded) + 3,)),
            pltpu.VMEM((256 + 2 * BORDER, D), BF16),
        ],
        name="local",
        compiler_params=pltpu.CompilerParams(vmem_limit_bytes=26 << 20),
        cost_estimate=pl.CostEstimate(
            flops=2 * 10**9, bytes_accessed=10 << 20, transcendentals=0
        ),
    )(*near, *in_hbm(loaded))
    return dict(zip(LOADED + ("middle", "received", "pre"), out))


def kept_shapes(rows):
    return [
        ((rows, 3 * D), BF16),
        ((rows, D), BF16),
        ((rows, D), F32),
        ((rows, D), F32),
        ((rows, 128), F32),
        ((256, D), BF16),
    ]


CHUNKS = ((64, 32, 256), BF16)


def nodes_kernel(
    from_west,
    from_east,
    centre,
    from_core,
    from_chip,
    owner,
    edge_sender,
    edge_receiver,
    nodes,
    edges,
    w_first,
    first_bias,
    w_second,
    norm_gain,
    mesh_cot,
    middle,
    received,
    pre_edge,
    updated_mesh_out,
    updated_edges_out,
    keep,
    send,
    x_edge,
    hid_edge,
    slope_edge,
    norm_edge,
    scale_edge,
    d_edge,
    x_grid,
    hid_grid,
    slope_grid,
    norm_grid,
    scale_grid,
    d_grid,
    x_node,
    hid_node,
    slope_node,
    norm_node,
    scale_node,
    updated_mesh,
    updated_edges,
    borders,
    sem,
):
    store_mesh = pltpu.make_async_copy(updated_mesh, updated_mesh_out, sem.at[0])
    store_edges = pltpu.make_async_copy(updated_edges, updated_edges_out, sem.at[1])
    n_nodes = nodes.shape[0]
    odd = lax.axis_index("c") == 1
    lower = jnp.where(odd, from_core[...], from_chip[...])
    upper = jnp.where(odd, from_chip[...], from_core[...])
    same = (from_west[0:SLOT_ROWS, :], centre[0:SLOT_ROWS, :], from_east[0:SLOT_ROWS, :])
    for block in range(9):
        rows = slice(block * CAP, (block + 1) * CAP)
        at = block % 3
        if block // 3 == 1:
            packet = same[at]
        else:
            packet = (lower, None, upper)[block // 3][at * SLOT_ROWS : (at + 1) * SLOT_ROWS, :]
        x_grid[rows, 0:D] = packet[0:CAP, :]
        x_grid[rows, D : 2 * D] = packet[CAP:SLOT_ROWS, :]
    borders[0:BORDER, :] = lower[3 * SLOT_ROWS :, :]
    borders[BORDER:, :] = upper[3 * SLOT_ROWS :, :]

    bordering = dot_tn(down_onehot(edge_sender[...] - n_nodes, 2 * BORDER), borders[...])
    x_edge[:, 0:D] = edges[...]
    x_edge[:, D : 2 * D] = (middle[...].astype(F32) + bordering).astype(BF16)
    x_edge[:, 2 * D :] = received[...]
    pre = pre_edge[...] + dot(x_edge[:, D : 2 * D], w_first[1, D : 2 * D, :])
    y_edge = forward(
        pre, w_second[1], norm_gain[1:2, :], slope_edge, hid_edge, norm_edge, scale_edge
    )
    updated_edges[...] = (edges[...].astype(F32) + y_edge).astype(BF16)
    store_edges.start()
    x_node[:, 2 * D :] = dot(
        down_onehot(edge_receiver[...], n_nodes), y_edge.astype(BF16)
    ).astype(BF16)

    owner_hot = down_onehot(owner[...], n_nodes)
    x_grid[:, 2 * D :] = dot_tn(owner_hot, nodes[...]).astype(BF16)
    pre = dot(x_grid[...], w_first[0]) + first_bias[0:1, :]
    y_grid = forward(
        pre, w_second[0], norm_gain[0:1, :], slope_grid, hid_grid, norm_grid, scale_grid
    )
    x_node[:, D : 2 * D] = dot(owner_hot, y_grid.astype(BF16)).astype(BF16)

    x_node[:, 0:D] = nodes[...]
    pre = dot(x_node[...], w_first[2]) + first_bias[2:3, :]
    gain = norm_gain[2:3, :]
    y_node = forward(pre, w_second[2], gain, slope_node, hid_node, norm_node, scale_node)
    updated_mesh[...] = (nodes[...].astype(F32) + y_node).astype(BF16)
    store_mesh.start()
    d_pre, d_out = backward(
        mesh_cot[...].astype(F32), w_second[2], gain, slope_node, norm_node, scale_node
    )
    d_grid[...] = dot_nt(d_pre, w_first[2, D : 2 * D, :]).astype(BF16)
    d_edge[...] = dot_nt(d_pre, w_first[2, 2 * D :, :]).astype(BF16)
    weight_grads(x_node, hid_node, d_pre, d_out, keep, send)
    store_edges.wait()
    store_mesh.wait()


def node_pass(*args):
    vmem = pl.BlockSpec(memory_space=pltpu.VMEM)
    hbm = pl.BlockSpec(memory_space=pltpu.HBM)
    outs = [CHUNKS, CHUNKS] + kept_shapes(512) + kept_shapes(288)
    return pl.pallas_call(
        nodes_kernel,
        out_shape=[
            jax.ShapeDtypeStruct((256, D), BF16),
            jax.ShapeDtypeStruct((512, D), BF16),
        ]
        + [jax.ShapeDtypeStruct(*shape) for shape in outs],
        in_specs=[vmem] * len(args),
        out_specs=[hbm, hbm] + [vmem] * len(outs),
        scratch_shapes=[pltpu.VMEM(*shape) for shape in kept_shapes(256)[:5]]
        + [
            pltpu.VMEM((256, D), BF16),
            pltpu.VMEM((512, D), BF16),
            pltpu.VMEM((2 * BORDER, D), BF16),
            pltpu.SemaphoreType.DMA((2,)),
        ],
        name="node_pass",
        compiler_params=pltpu.CompilerParams(vmem_limit_bytes=22 << 20),
        cost_estimate=pl.CostEstimate(
            flops=4 * 10**9, bytes_accessed=20 << 20, transcendentals=10**6
        ),
    )(*args)


def edge_pass(k, index, cotangent, w_second, norm_gain, kept):
    given = () if cotangent is None else (cotangent,)

    def kernel(index, w_second, norm_gain, x, hid, slope, norm, scale, d_sum, *refs):
        keep, send = refs[-2:]
        dy = dot_tn(down_onehot(index[...], d_sum.shape[0]), d_sum[...])
        if given:
            dy = refs[0][...].astype(F32) + dy
        d_pre, d_out = backward(dy, w_second[k], norm_gain[k : k + 1, :], slope, norm, scale)
        weight_grads(x, hid, d_pre, d_out, keep, send)

    vmem = pl.BlockSpec(memory_space=pltpu.VMEM)
    args = (index, w_second, norm_gain, *kept, *given)
    return pl.pallas_call(
        kernel,
        out_shape=[jax.ShapeDtypeStruct(*CHUNKS)] * 2,
        in_specs=[vmem] * len(args),
        out_specs=[vmem] * 2,
        compiler_params=pltpu.CompilerParams(vmem_limit_bytes=24 << 20),
        cost_estimate=pl.CostEstimate(
            flops=2 * 10**9, bytes_accessed=8 << 20, transcendentals=10**4
        ),
    )(*args)


def this_place():
    return [lax.axis_index(axis) for axis in ("c", "z", "x", "y")]


def small_call(kernel, shapes, *args):
    vmem = pl.BlockSpec(memory_space=pltpu.VMEM)
    moved = sum(a.size * 2 for a in args)
    return pl.pallas_call(
        kernel,
        out_shape=[jax.ShapeDtypeStruct(shape, dtype) for shape, dtype in shapes],
        in_specs=[vmem] * len(args),
        out_specs=[vmem] * len(shapes),
        compiler_params=pltpu.CompilerParams(vmem_limit_bytes=12 << 20),
        cost_estimate=pl.CostEstimate(flops=moved, bytes_accessed=moved, transcendentals=0),
    )(*args)


Z, X, Y = 1, 2, 3
AXES = {0: (Y, X, Z), 1: (X, Z, Y), 2: (Z, Y, X)}


def masks(place):
    return 1 + 2 * place[0], 3 - 2 * place[0]


def partner_pairs(axis, second):
    pairs = []
    for device in range(128):
        z, c, x, y = device >> 5, (device >> 4) & 1, (device >> 2) & 3, device & 3
        mask = (3 - 2 * c) if second else (1 + 2 * c)
        at = {Z: z, X: x, Y: y}
        at[axis] ^= mask
        pairs.append((device, ((at[Z] * 2 + c) * 4 + at[X]) * 4 + at[Y]))
    return pairs


def swap_along(value, axis, second):
    return lax.ppermute(value, ALL, partner_pairs(axis, second))


def chunk_at(left, axis, i, r):
    n = len(left)
    stride = 4 ** (n - 1 - left.index(axis))
    low = r & (stride - 1)
    return (r - low) * 4 + i * stride + low


def halve(k, step, *inputs):
    axis = AXES[k][step]
    left = sorted(AXES[k][step:])
    count = 4 ** (len(left) - 1)

    def kernel(a, b, kept, sent):
        place = this_place()
        m1, m2 = masks(place)
        mine = place[axis]
        for out, base in ((kept, mine), (sent, mine ^ m1)):
            for j in range(2):
                i = base ^ (m2 * j)

                def body(r, carry):
                    at = chunk_at(left, axis, i, r)
                    out[j, r] = a[at] + b[at]
                    return carry

                lax.fori_loop(0, count, body, 0, unroll=min(count, 8))

    half = ((2, count, 32, 256), BF16)
    return small_call(kernel, (half, half), *inputs)


def quarter(kept, got):
    count = kept.shape[1]

    def kernel(kept, got, keep, send):
        for j, out in ((0, keep), (1, send)):

            def body(r, carry):
                out[r] = kept[j, r] + got[j, r]
                return carry

            lax.fori_loop(0, count, body, 0, unroll=min(count, 8))

    half = ((count, 32, 256), BF16)
    return small_call(kernel, (half, half), kept, got)


def reduced(k, keep, got):
    for step, axis in enumerate(AXES[k]):
        keep, send = halve(k, step, keep, got)
        got = swap_along(send, axis, False)
        keep, send = quarter(keep, got)
        got = swap_along(send, axis, True)
    return keep, got


def finish(terms):
    def kernel(*refs):
        grad_first, grad_second = refs[6:]
        odd = lax.axis_index("c") == 1
        for k in range(3):
            total = refs[2 * k][0].astype(F32) + refs[2 * k + 1][0].astype(F32)
            turned = pltpu.roll(total, 64, 1)
            grad_first[k] = jnp.where(odd, turned, total)[:, 0:192]
            grad_second[k] = jnp.where(odd, total[:, 128:192], turned[:, 0:64])

    shapes = (((3, 32, 192), F32), ((3, 32, 64), F32))
    return small_call(kernel, shapes, *[t for pair in terms for t in pair])


def shards(
    grid_nodes,
    grid_edges,
    grid_sender,
    owner_index,
    mesh_nodes,
    mesh_edges,
    mesh_sender,
    mesh_receiver,
    w_first,
    first_bias,
    w_second,
    norm_gain,
    mesh_cotangent,
    edge_cotangent,
):
    lats = lax.axis_size(LAT)
    lons = lax.axis_size(LON)
    swap = [(0, 1), (1, 0)]
    east, west, middle, coarse = packets(grid_nodes, grid_edges, grid_sender, mesh_nodes)
    from_west = lax.ppermute(east, ALL, lon_pairs(1, lats, lons))
    from_east = lax.ppermute(west, ALL, lon_pairs(-1, lats, lons))
    coarse_own = lax.all_to_all(coarse, ("z", "x", "y"), 0, 0, tiled=True)
    coarse_own = coarse_own.reshape(-1, D // 2)
    to_core, to_chip = relay(from_west, from_east, middle)
    from_chip = lax.ppermute(to_chip, ALL, chip_pairs(lats, lons))
    from_core = lax.ppermute(to_core, "c", swap)
    coarse_other = lax.ppermute(coarse_own, "c", swap)
    at = local(
        (from_west, from_east, coarse_own, coarse_other),
        (
            mesh_receiver,
            mesh_sender,
            mesh_nodes,
            w_first,
            mesh_edges,
            first_bias,
            owner_index,
            norm_gain,
            w_second,
            mesh_cotangent,
            edge_cotangent,
        ),
    )
    updated_mesh, updated_edges, keep, send, *kept = node_pass(
        from_west,
        from_east,
        middle,
        from_core,
        from_chip,
        at["owner"],
        at["mesh_sender"],
        at["edge_receiver"],
        at["nodes"],
        at["edges"],
        at["w_first"],
        at["first_bias"],
        at["w_second"],
        at["norm_gain"],
        at["mesh_cot"],
        at["middle"],
        at["received"],
        at["pre"],
    )
    terms = {2: reduced(2, keep, lax.ppermute(send, "c", swap))}
    for k, index, cotangent, saved in (
        (1, at["edge_receiver"], at["edge_cot"], kept[:6]),
        (0, at["owner"], None, kept[6:]),
    ):
        keep, send = edge_pass(k, index, cotangent, at["w_second"], at["norm_gain"], saved)
        terms[k] = reduced(k, keep, lax.ppermute(send, "c", swap))
    first, second = finish([terms[k] for k in range(3)])
    return (updated_mesh, updated_edges, first.transpose(0, 2, 1), second.transpose(0, 2, 1))


def solution(mesh):
    finer = Mesh(mesh.devices.reshape(4, 2, 4, 4), ALL)
    by_device = P(ALL, None)
    index = P(ALL)

    return jax.shard_map(
        shards,
        mesh=finer,
        in_specs=(
            by_device,
            by_device,
            index,
            index,
            by_device,
            by_device,
            index,
            index,
            P(),
            P(),
            P(),
            P(),
            by_device,
            by_device,
        ),
        out_specs=(by_device, by_device, P(None, LAT, LON), P(None, LAT, LON)),
        check_vma=False,
    )
```

```python
import jax
import jax.numpy as jnp
from jax import lax
from jax.experimental import pallas as pl
from jax.experimental.pallas import tpu as pltpu
from jax.sharding import Mesh
from jax.sharding import PartitionSpec as P

D = 512
CAP = 32
BORDER = 64
K_COARSE = 4
EPSILON = 1e-05
ALL = ("z", "c", "x", "y")
LAT = ("z", "c")
LON = ("x", "y")
F32 = jnp.float32
BF16 = jnp.bfloat16


SLOT_ROWS = 2 * CAP
PACKET = 3 * SLOT_ROWS + BORDER


def lon_pairs(by, lats, lons):
    return [
        (lat * lons + lon, lat * lons + (lon + by) % lons)
        for lat in range(lats)
        for lon in range(lons)
    ]


def chip_pairs(lats, lons):
    pairs = []
    for lat in range(1, lats - 1, 2):
        for lon in range(lons):
            lower, upper = lat * lons + lon, (lat + 1) * lons + lon
            pairs += [(lower, upper), (upper, lower)]
    return pairs


def in_hbm(arrays):
    return [pltpu.with_memory_space_constraint(a, pltpu.HBM) for a in arrays]


def dot(a, b):
    return jnp.dot(a, b, preferred_element_type=F32)


def dot_nt(a, b):
    return lax.dot_general(a, b, (((1,), (1,)), ((), ())), preferred_element_type=F32)


def dot_tn(a, b):
    return lax.dot_general(a, b, (((0,), (0,)), ((), ())), preferred_element_type=F32)


def down_onehot(index, count):
    index = index.reshape(1, -1)
    lines = lax.broadcasted_iota(jnp.int32, (count, index.shape[1]), 0)
    return jnp.where(lines == index, 1.0, 0.0).astype(BF16)


def coarse_line(row):
    at = row - 512
    device = at >> 2
    chip = ((device >> 5) << 4) + (device & 15)
    other = ((device >> 4) & 1) ^ lax.axis_index("c")
    return jnp.where(at < 0, -2 * K_COARSE, other * 512 + chip * 8 + (at & 3))


def pack_kernel(*refs):
    hbm, (east, west, middle, coarse), (picked, sem), local = (
        refs[:4],
        refs[4:8],
        refs[8:10],
        refs[10:],
    )
    loads = [
        pltpu.make_async_copy(source, to, sem.at[i])
        for i, (source, to) in enumerate(zip(hbm, local))
    ]
    for load in loads:
        load.start()
    for load in loads:
        load.wait()
    points, slot_edges, senders, nodes = local
    picked[...] = dot_tn(down_onehot(senders[...], points.shape[0]), points[...]).astype(BF16)
    toward_core = jnp.where(lax.axis_index("c") == 1, 0, 2)
    bands = (1, toward_core, 2 - toward_core)
    for column, out in ((2, east), (0, west), (1, middle)):
        for at, band in enumerate(bands):
            block = pl.multiple_of((band * 3 + column) * CAP, CAP)
            to = at * SLOT_ROWS
            out[to : to + CAP, :] = slot_edges[pl.ds(block, CAP), :]
            out[to + CAP : to + SLOT_ROWS, :] = picked[pl.ds(block, CAP), :]
        out[3 * SLOT_ROWS : PACKET, :] = nodes[0:BORDER, :]
    rows = nodes[nodes.shape[0] - 8 :, :].astype(F32)[8 - K_COARSE :, :]
    halves = jnp.concatenate([rows[:, : D // 2], rows[:, D // 2 :]], axis=0).astype(BF16)
    coarse[...] = jnp.broadcast_to(halves[None], coarse.shape)


def packets(points, slot_edges, senders, nodes):
    packet = jax.ShapeDtypeStruct((PACKET, D), BF16)
    vmem = pl.BlockSpec(memory_space=pltpu.VMEM)
    return pl.pallas_call(
        pack_kernel,
        out_shape=[packet] * 3 + [jax.ShapeDtypeStruct((64, 2 * K_COARSE, D // 2), BF16)],
        in_specs=[pl.BlockSpec(memory_space=pltpu.HBM)] * 4,
        out_specs=[vmem] * 4,
        scratch_shapes=[pltpu.VMEM((9 * CAP, D), BF16), pltpu.SemaphoreType.DMA((4,))]
        + [pltpu.VMEM(a.shape, a.dtype) for a in (points, slot_edges, senders, nodes)],
        name="pack",
        compiler_params=pltpu.CompilerParams(vmem_limit_bytes=16 << 20),
        cost_estimate=pl.CostEstimate(
            flops=2 * 288 * 1024 * 512, bytes_accessed=2 << 20, transcendentals=0
        ),
    )(*in_hbm((points, slot_edges, senders, nodes)))


def relay_kernel(from_west, from_east, middle, to_core, to_chip):
    for at, out in ((1, to_core), (2, to_chip)):
        rows = slice(at * SLOT_ROWS, (at + 1) * SLOT_ROWS)
        for i, source in enumerate((from_west, middle, from_east)):
            out[i * SLOT_ROWS : (i + 1) * SLOT_ROWS, :] = source[rows, :]
        out[3 * SLOT_ROWS : PACKET, :] = middle[3 * SLOT_ROWS : PACKET, :]


def relay(from_west, from_east, middle):
    vmem = pl.BlockSpec(memory_space=pltpu.VMEM)
    return pl.pallas_call(
        relay_kernel,
        out_shape=[jax.ShapeDtypeStruct((PACKET, D), BF16)] * 2,
        in_specs=[vmem] * 3,
        out_specs=[vmem] * 2,
        name="relay",
        compiler_params=pltpu.CompilerParams(vmem_limit_bytes=16 << 20),
        cost_estimate=pl.CostEstimate(flops=10**6, bytes_accessed=1 << 20, transcendentals=0),
    )(from_west, from_east, middle)


def forward(pre, w_second, gain, slope, hid, norm, scale):
    sig = 0.5 + 0.5 * jnp.tanh(0.5 * pre)
    act = pre * sig
    hid[...] = act.astype(BF16)
    slope[...] = sig + act * (1.0 - sig)
    out = dot(hid[...], w_second)
    out = out - jnp.mean(out, axis=1, keepdims=True)
    size = lax.rsqrt(jnp.mean(out * out, axis=1, keepdims=True) + EPSILON)
    scale[...] = jnp.broadcast_to(size, scale.shape)
    unit = out * size
    norm[...] = unit
    return unit * gain


def backward(dy, w_second, gain, slope, norm, scale):
    unit = norm[...]
    dn = dy * gain
    mid = jnp.mean(dn, axis=1, keepdims=True)
    along = jnp.mean(dn * unit, axis=1, keepdims=True)
    d_out = (scale[:, 0:1] * (dn - mid - unit * along)).astype(BF16)
    d_hid = dot_nt(d_out, w_second).astype(BF16)
    d_pre = (d_hid.astype(F32) * slope[...]).astype(BF16)
    return d_pre, d_out


def weight_grads(x, hid, d_pre, d_out, keep, send):
    odd = lax.axis_index("c") == 1
    low = lax.broadcasted_iota(jnp.int32, (D, 128), 1) < 64
    second = dot_tn(d_out, hid[...])
    for z in range(4):
        first = dot_tn(d_pre, x[:, 384 * z : 384 * (z + 1)])
        turned = pltpu.roll(second[:, 128 * z : 128 * (z + 1)], 64, 1)
        middle = first[:, 128:256]
        even_a, odd_a = first[:, 0:128], first[:, 256:384]
        even_b = jnp.where(low, middle, turned)
        odd_b = jnp.where(low, turned, middle)
        for ref, a, b in (
            (keep, jnp.where(odd, odd_a, even_a), jnp.where(odd, odd_b, even_b)),
            (send, jnp.where(odd, even_a, odd_a), jnp.where(odd, even_b, odd_b)),
        ):
            ref[16 * z : 16 * (z + 1), :, 0:128] = a.astype(BF16).reshape(16, 32, 128)
            ref[16 * z : 16 * (z + 1), :, 128:256] = b.astype(BF16).reshape(16, 32, 128)


LOADED = (
    "edge_receiver",
    "mesh_sender",
    "nodes",
    "w_first",
    "edges",
    "first_bias",
    "owner",
    "norm_gain",
    "w_second",
    "mesh_cot",
    "edge_cot",
)


def local_kernel(from_west, from_east, *refs):
    n = len(LOADED)
    hbm, vmem = refs[:n], refs[n : 2 * n]
    middle, received, pre, sem, table = refs[2 * n :]
    to = dict(zip(LOADED, vmem))
    loads = {
        name: pltpu.make_async_copy(source, target, sem.at[i])
        for i, (name, source, target) in enumerate(zip(LOADED, hbm, vmem))
        if name != "w_first"
    }
    w_first = dict(zip(LOADED, hbm))["w_first"]
    for k in range(3):
        loads[f"w_first_{k}"] = pltpu.make_async_copy(
            w_first.at[k], to["w_first"].at[k], sem.at[n + k]
        )
    for name in ("edge_receiver", "mesh_sender", "nodes", "w_first_1", "edges", "first_bias"):
        loads[name].start()
    rest = [name for name in loads if name in ("owner", "norm_gain", "w_second", "mesh_cot", "edge_cot")]
    rest += ["w_first_0", "w_first_2"]
    for name in rest:
        loads[name].start()
    for name in ("edge_receiver", "mesh_sender", "nodes"):
        loads[name].wait()
    nodes = to["nodes"]
    n_nodes = nodes.shape[0]
    table[0:n_nodes, :] = nodes[...]
    table[n_nodes : n_nodes + BORDER, :] = from_west[3 * SLOT_ROWS :, :]
    table[n_nodes + BORDER :, :] = from_east[3 * SLOT_ROWS :, :]
    sender = to["mesh_sender"][...]
    late = sender - 2 * BORDER
    line = jnp.where(sender < n_nodes, sender, jnp.where(late < n_nodes, -1, late))
    middle[...] = dot_tn(down_onehot(line, table.shape[0]), table[...]).astype(BF16)
    received[...] = dot_tn(down_onehot(to["edge_receiver"][...], n_nodes), nodes[...]).astype(BF16)
    for name in ("w_first_1", "edges", "first_bias"):
        loads[name].wait()
    w = to["w_first"]
    pre[...] = (
        dot(to["edges"][...], w[1, 0:D, :])
        + dot(received[...], w[1, 2 * D :, :])
        + to["first_bias"][1:2, :]
    )
    for name in rest:
        loads[name].wait()


def local(near, loaded):
    vmem = pl.BlockSpec(memory_space=pltpu.VMEM)
    hbm = pl.BlockSpec(memory_space=pltpu.HBM)
    out = pl.pallas_call(
        local_kernel,
        out_shape=[jax.ShapeDtypeStruct(a.shape, a.dtype) for a in loaded]
        + [
            jax.ShapeDtypeStruct((512, D), BF16),
            jax.ShapeDtypeStruct((512, D), BF16),
            jax.ShapeDtypeStruct((512, D), F32),
        ],
        in_specs=[vmem] * len(near) + [hbm] * len(loaded),
        out_specs=[vmem] * (len(loaded) + 3),
        scratch_shapes=[
            pltpu.SemaphoreType.DMA((len(loaded) + 3,)),
            pltpu.VMEM((256 + 2 * BORDER, D), BF16),
        ],
        name="local",
        compiler_params=pltpu.CompilerParams(vmem_limit_bytes=26 << 20),
        cost_estimate=pl.CostEstimate(
            flops=2 * 10**9, bytes_accessed=10 << 20, transcendentals=0
        ),
    )(*near, *in_hbm(loaded))
    return dict(zip(LOADED + ("middle", "received", "pre"), out))


def kept_shapes(rows):
    return [
        ((rows, 3 * D), BF16),
        ((rows, D), BF16),
        ((rows, D), F32),
        ((rows, D), F32),
        ((rows, 128), F32),
        ((256, D), BF16),
    ]


CHUNKS = ((64, 32, 256), BF16)


def nodes_kernel(
    from_west,
    from_east,
    centre,
    from_core,
    from_chip,
    coarse_own,
    coarse_other,
    owner,
    edge_sender,
    edge_receiver,
    nodes,
    edges,
    w_first,
    first_bias,
    w_second,
    norm_gain,
    mesh_cot,
    middle,
    received,
    pre_edge,
    updated_mesh_out,
    updated_edges_out,
    keep,
    send,
    x_edge,
    hid_edge,
    slope_edge,
    norm_edge,
    scale_edge,
    d_edge,
    x_grid,
    hid_grid,
    slope_grid,
    norm_grid,
    scale_grid,
    d_grid,
    x_node,
    hid_node,
    slope_node,
    norm_node,
    scale_node,
    updated_mesh,
    updated_edges,
    borders,
    sem,
):
    store_mesh = pltpu.make_async_copy(updated_mesh, updated_mesh_out, sem.at[0])
    store_edges = pltpu.make_async_copy(updated_edges, updated_edges_out, sem.at[1])
    n_nodes = nodes.shape[0]
    odd = lax.axis_index("c") == 1
    lower = jnp.where(odd, from_core[...], from_chip[...])
    upper = jnp.where(odd, from_chip[...], from_core[...])
    same = (from_west[0:SLOT_ROWS, :], centre[0:SLOT_ROWS, :], from_east[0:SLOT_ROWS, :])
    for block in range(9):
        rows = slice(block * CAP, (block + 1) * CAP)
        at = block % 3
        if block // 3 == 1:
            packet = same[at]
        else:
            packet = (lower, None, upper)[block // 3][at * SLOT_ROWS : (at + 1) * SLOT_ROWS, :]
        x_grid[rows, 0:D] = packet[0:CAP, :]
        x_grid[rows, D : 2 * D] = packet[CAP:SLOT_ROWS, :]
    borders[0:BORDER, :] = lower[3 * SLOT_ROWS :, :]
    borders[BORDER:, :] = upper[3 * SLOT_ROWS :, :]

    sender = edge_sender[...]
    near = middle[...].astype(F32)
    near = near + dot_tn(down_onehot(sender - n_nodes, 2 * BORDER), borders[...])
    line = coarse_line(sender)
    halves = coarse_own.shape[0]
    for half in range(2):
        hot = down_onehot(line + half * K_COARSE, 2 * halves)
        part = dot_tn(hot[:halves], coarse_own[...]) + dot_tn(hot[halves:], coarse_other[...])
        to = slice(D + 256 * half, D + 256 * (half + 1))
        x_edge[:, to] = (near[:, 256 * half : 256 * (half + 1)] + part).astype(BF16)
    x_edge[:, 0:D] = edges[...]
    x_edge[:, 2 * D :] = received[...]
    pre = pre_edge[...] + dot(x_edge[:, D : 2 * D], w_first[1, D : 2 * D, :])
    y_edge = forward(
        pre, w_second[1], norm_gain[1:2, :], slope_edge, hid_edge, norm_edge, scale_edge
    )
    updated_edges[...] = (edges[...].astype(F32) + y_edge).astype(BF16)
    store_edges.start()
    x_node[:, 2 * D :] = dot(
        down_onehot(edge_receiver[...], n_nodes), y_edge.astype(BF16)
    ).astype(BF16)

    owner_hot = down_onehot(owner[...], n_nodes)
    x_grid[:, 2 * D :] = dot_tn(owner_hot, nodes[...]).astype(BF16)
    pre = dot(x_grid[...], w_first[0]) + first_bias[0:1, :]
    y_grid = forward(
        pre, w_second[0], norm_gain[0:1, :], slope_grid, hid_grid, norm_grid, scale_grid
    )
    x_node[:, D : 2 * D] = dot(owner_hot, y_grid.astype(BF16)).astype(BF16)

    x_node[:, 0:D] = nodes[...]
    pre = dot(x_node[...], w_first[2]) + first_bias[2:3, :]
    gain = norm_gain[2:3, :]
    y_node = forward(pre, w_second[2], gain, slope_node, hid_node, norm_node, scale_node)
    updated_mesh[...] = (nodes[...].astype(F32) + y_node).astype(BF16)
    store_mesh.start()
    d_pre, d_out = backward(
        mesh_cot[...].astype(F32), w_second[2], gain, slope_node, norm_node, scale_node
    )
    d_grid[...] = dot_nt(d_pre, w_first[2, D : 2 * D, :]).astype(BF16)
    d_edge[...] = dot_nt(d_pre, w_first[2, 2 * D :, :]).astype(BF16)
    weight_grads(x_node, hid_node, d_pre, d_out, keep, send)
    store_edges.wait()
    store_mesh.wait()


def node_pass(*args):
    vmem = pl.BlockSpec(memory_space=pltpu.VMEM)
    hbm = pl.BlockSpec(memory_space=pltpu.HBM)
    outs = [CHUNKS, CHUNKS] + kept_shapes(512) + kept_shapes(288)
    return pl.pallas_call(
        nodes_kernel,
        out_shape=[
            jax.ShapeDtypeStruct((256, D), BF16),
            jax.ShapeDtypeStruct((512, D), BF16),
        ]
        + [jax.ShapeDtypeStruct(*shape) for shape in outs],
        in_specs=[vmem] * len(args),
        out_specs=[hbm, hbm] + [vmem] * len(outs),
        scratch_shapes=[pltpu.VMEM(*shape) for shape in kept_shapes(256)[:5]]
        + [
            pltpu.VMEM((256, D), BF16),
            pltpu.VMEM((512, D), BF16),
            pltpu.VMEM((2 * BORDER, D), BF16),
            pltpu.SemaphoreType.DMA((2,)),
        ],
        name="node_pass",
        compiler_params=pltpu.CompilerParams(vmem_limit_bytes=22 << 20),
        cost_estimate=pl.CostEstimate(
            flops=4 * 10**9, bytes_accessed=20 << 20, transcendentals=10**6
        ),
    )(*args)


def edge_pass(k, index, cotangent, w_second, norm_gain, kept):
    given = () if cotangent is None else (cotangent,)

    def kernel(index, w_second, norm_gain, x, hid, slope, norm, scale, d_sum, *refs):
        keep, send = refs[-2:]
        dy = dot_tn(down_onehot(index[...], d_sum.shape[0]), d_sum[...])
        if given:
            dy = refs[0][...].astype(F32) + dy
        d_pre, d_out = backward(dy, w_second[k], norm_gain[k : k + 1, :], slope, norm, scale)
        weight_grads(x, hid, d_pre, d_out, keep, send)

    vmem = pl.BlockSpec(memory_space=pltpu.VMEM)
    args = (index, w_second, norm_gain, *kept, *given)
    return pl.pallas_call(
        kernel,
        out_shape=[jax.ShapeDtypeStruct(*CHUNKS)] * 2,
        in_specs=[vmem] * len(args),
        out_specs=[vmem] * 2,
        compiler_params=pltpu.CompilerParams(vmem_limit_bytes=24 << 20),
        cost_estimate=pl.CostEstimate(
            flops=2 * 10**9, bytes_accessed=8 << 20, transcendentals=10**4
        ),
    )(*args)


def this_place():
    return [lax.axis_index(axis) for axis in ("c", "z", "x", "y")]


def small_call(kernel, shapes, *args):
    vmem = pl.BlockSpec(memory_space=pltpu.VMEM)
    moved = sum(a.size * 2 for a in args)
    return pl.pallas_call(
        kernel,
        out_shape=[jax.ShapeDtypeStruct(shape, dtype) for shape, dtype in shapes],
        in_specs=[vmem] * len(args),
        out_specs=[vmem] * len(shapes),
        compiler_params=pltpu.CompilerParams(vmem_limit_bytes=12 << 20),
        cost_estimate=pl.CostEstimate(flops=moved, bytes_accessed=moved, transcendentals=0),
    )(*args)


Z, X, Y = 1, 2, 3
AXES = {0: (Y, X, Z), 1: (X, Z, Y), 2: (Z, Y, X)}


def masks(place):
    return 1 + 2 * place[0], 3 - 2 * place[0]


def partner_pairs(axis, second):
    pairs = []
    for device in range(128):
        z, c, x, y = device >> 5, (device >> 4) & 1, (device >> 2) & 3, device & 3
        mask = (3 - 2 * c) if second else (1 + 2 * c)
        at = {Z: z, X: x, Y: y}
        at[axis] ^= mask
        pairs.append((device, ((at[Z] * 2 + c) * 4 + at[X]) * 4 + at[Y]))
    return pairs


def swap_along(value, axis, second):
    return lax.ppermute(value, ALL, partner_pairs(axis, second))


def chunk_at(left, axis, i, r):
    n = len(left)
    stride = 4 ** (n - 1 - left.index(axis))
    low = r & (stride - 1)
    return (r - low) * 4 + i * stride + low


def halve(k, step, *inputs):
    axis = AXES[k][step]
    left = sorted(AXES[k][step:])
    count = 4 ** (len(left) - 1)

    def kernel(a, b, kept, sent):
        place = this_place()
        m1, m2 = masks(place)
        mine = place[axis]
        for out, base in ((kept, mine), (sent, mine ^ m1)):
            for j in range(2):
                i = base ^ (m2 * j)

                def body(r, carry):
                    at = chunk_at(left, axis, i, r)
                    out[j, r] = a[at] + b[at]
                    return carry

                lax.fori_loop(0, count, body, 0, unroll=min(count, 8))

    half = ((2, count, 32, 256), BF16)
    return small_call(kernel, (half, half), *inputs)


def quarter(kept, got):
    count = kept.shape[1]

    def kernel(kept, got, keep, send):
        for j, out in ((0, keep), (1, send)):

            def body(r, carry):
                out[r] = kept[j, r] + got[j, r]
                return carry

            lax.fori_loop(0, count, body, 0, unroll=min(count, 8))

    half = ((count, 32, 256), BF16)
    return small_call(kernel, (half, half), kept, got)


def reduced(k, keep, got):
    for step, axis in enumerate(AXES[k]):
        keep, send = halve(k, step, keep, got)
        got = swap_along(send, axis, False)
        keep, send = quarter(keep, got)
        got = swap_along(send, axis, True)
    return keep, got


def finish(terms):
    def kernel(*refs):
        grad_first, grad_second = refs[6:]
        odd = lax.axis_index("c") == 1
        for k in range(3):
            total = refs[2 * k][0].astype(F32) + refs[2 * k + 1][0].astype(F32)
            turned = pltpu.roll(total, 64, 1)
            grad_first[k] = jnp.where(odd, turned, total)[:, 0:192]
            grad_second[k] = jnp.where(odd, total[:, 128:192], turned[:, 0:64])

    shapes = (((3, 32, 192), F32), ((3, 32, 64), F32))
    return small_call(kernel, shapes, *[t for pair in terms for t in pair])


def shards(
    grid_nodes,
    grid_edges,
    grid_sender,
    owner_index,
    mesh_nodes,
    mesh_edges,
    mesh_sender,
    mesh_receiver,
    w_first,
    first_bias,
    w_second,
    norm_gain,
    mesh_cotangent,
    edge_cotangent,
):
    lats = lax.axis_size(LAT)
    lons = lax.axis_size(LON)
    swap = [(0, 1), (1, 0)]
    east, west, middle, coarse = packets(grid_nodes, grid_edges, grid_sender, mesh_nodes)
    from_west = lax.ppermute(east, ALL, lon_pairs(1, lats, lons))
    from_east = lax.ppermute(west, ALL, lon_pairs(-1, lats, lons))
    coarse_own = lax.all_to_all(coarse, ("z", "x", "y"), 0, 0, tiled=True)
    coarse_own = coarse_own.reshape(-1, D // 2)
    to_core, to_chip = relay(from_west, from_east, middle)
    from_chip = lax.ppermute(to_chip, ALL, chip_pairs(lats, lons))
    from_core = lax.ppermute(to_core, "c", swap)
    coarse_other = lax.ppermute(coarse_own, "c", swap)
    at = local(
        (from_west, from_east),
        (
            mesh_receiver,
            mesh_sender,
            mesh_nodes,
            w_first,
            mesh_edges,
            first_bias,
            owner_index,
            norm_gain,
            w_second,
            mesh_cotangent,
            edge_cotangent,
        ),
    )
    updated_mesh, updated_edges, keep, send, *kept = node_pass(
        from_west,
        from_east,
        middle,
        from_core,
        from_chip,
        coarse_own,
        coarse_other,
        at["owner"],
        at["mesh_sender"],
        at["edge_receiver"],
        at["nodes"],
        at["edges"],
        at["w_first"],
        at["first_bias"],
        at["w_second"],
        at["norm_gain"],
        at["mesh_cot"],
        at["middle"],
        at["received"],
        at["pre"],
    )
    terms = {2: reduced(2, keep, lax.ppermute(send, "c", swap))}
    for k, index, cotangent, saved in (
        (1, at["edge_receiver"], at["edge_cot"], kept[:6]),
        (0, at["owner"], None, kept[6:]),
    ):
        keep, send = edge_pass(k, index, cotangent, at["w_second"], at["norm_gain"], saved)
        terms[k] = reduced(k, keep, lax.ppermute(send, "c", swap))
    first, second = finish([terms[k] for k in range(3)])
    return (updated_mesh, updated_edges, first.transpose(0, 2, 1), second.transpose(0, 2, 1))


def solution(mesh):
    finer = Mesh(mesh.devices.reshape(4, 2, 4, 4), ALL)
    by_device = P(ALL, None)
    index = P(ALL)

    return jax.shard_map(
        shards,
        mesh=finer,
        in_specs=(
            by_device,
            by_device,
            index,
            index,
            by_device,
            by_device,
            index,
            index,
            P(),
            P(),
            P(),
            P(),
            by_device,
            by_device,
        ),
        out_specs=(by_device, by_device, P(None, LAT, LON), P(None, LAT, LON)),
        check_vma=False,
    )
```
